16 devices in a mesh: dp: 2 (over y, z), tp: 8 (over x, core).
Axes of the slice: x: 4, y: 2, z: 1, core: 2. Of those that a mesh axis runs over, the one named last changes fastest.
The devices are a block of a 4x4x8 slice.
Arguments:
- hidden: bfloat16 [8192, 768], P(('dp', 'tp')), parts along dimension 0
- targets: int32 [8192], P(('dp', 'tp')), parts along dimension 0
- loss_mask: int32 [8192], P(('dp', 'tp')), parts along dimension 0
- ln_params: float32 [2, 768], replicated
- out_embed: bfloat16 [50304, 768], P('tp')
- ln_mom1: float32 [2, 768], replicated
- ln_mom2: float32 [2, 768], replicated
- embed_mom1: float32 [50304, 768], P('tp')
- embed_mom2: float32 [50304, 768], P('tp')
Outputs:
- output 1: float32 [8192], P(('dp', 'tp')), parts along dimension 0
- output 2: float32 [2], P('dp'), parts along dimension 0
- output 3: bfloat16 [8192, 768], P(('dp', 'tp')), parts along dimension 0
- output 4: float32 [4, 768], P('dp'), parts along dimension 0
- output 5: float32 [4, 768], P('dp'), parts along dimension 0
- output 6: float32 [4, 768], P('dp'), parts along dimension 0
- output 7: bfloat16 [100608, 768], P(('dp', 'tp')), parts along dimension 0
- output 8: float32 [100608, 768], P(('dp', 'tp')), parts along dimension 0
- output 9: float32 [100608, 768], P(('dp', 'tp')), parts along dimension 0
There are 2 independent parts. The reference program is written for one: setup_inputs(seed, part) draws one part's arguments, and reference() takes and returns one part's arrays. A program takes and returns all parts, laid end to end along the dimension named above; an argument that names none is the same for every part.
All inputs are finite; a program needn't handle non-finite values.
Results may differ from the reference program's by a relative error of at most 0.001.
Values are sent between devices in bfloat16 or wider.
A program may use at most 768 MiB of HBM per device.

```python
import math
import jax
import jax.numpy as jnp
from jax import lax

MODEL_DIM = 768
VOCAB_SIZE = 50304
SEQ_LEN = 4096
ADAM_STEP = 10
ROW_BLOCK = math.gcd(SEQ_LEN, 256)
NUM_BLOCKS = SEQ_LEN // ROW_BLOCK
LN_EPS = 1e-5
BETA_ONE = 0.9
BETA_TWO = 0.95
ADAM_EPS = 1e-8
LEARN_RATE = 1e-3
WEIGHT_DECAY = 0.1


def setup_inputs(seed: int = 0, part: int = 0) -> dict:
    root_key = jax.random.key(seed)
    shared_keys = jax.random.split(root_key, 6)
    part_keys = jax.random.split(jax.random.fold_in(root_key, part), 4)
    hidden = jax.random.normal(part_keys[0], (SEQ_LEN, MODEL_DIM), jnp.float32).astype(jnp.bfloat16)
    targets = jax.random.randint(part_keys[1], (SEQ_LEN,), 0, VOCAB_SIZE, jnp.int32)
    keep_bits = jax.random.randint(part_keys[2], (SEQ_LEN,), 0, 4, jnp.int32)
    pad_len = jax.random.randint(part_keys[3], (), 0, SEQ_LEN // 4, jnp.int32)
    positions = jnp.arange(SEQ_LEN, dtype=jnp.int32)
    keep_tok = (keep_bits > 0) & (positions < SEQ_LEN - pad_len)
    loss_mask = jnp.where(positions == 0, 1, keep_tok.astype(jnp.int32)).astype(jnp.int32)
    embed_scale = 2.3 * MODEL_DIM ** -0.5
    out_embed = (jax.random.normal(shared_keys[0], (VOCAB_SIZE, MODEL_DIM), jnp.float32) * embed_scale).astype(jnp.bfloat16)
    ln_noise = jax.random.normal(shared_keys[1], (2, MODEL_DIM), jnp.float32)
    ln_params = jnp.stack([1.0 + 0.3 * ln_noise[0], 0.3 * ln_noise[1]])
    valid_est = 0.66 * SEQ_LEN
    embed_grad = (valid_est * VOCAB_SIZE) ** -0.5
    ln_grad = 2.3 * (valid_est * MODEL_DIM) ** -0.5
    ln_mom1 = jax.random.normal(shared_keys[2], (2, MODEL_DIM), jnp.float32) * ln_grad
    ln_mom2 = (0.5 + jax.random.uniform(shared_keys[3], (2, MODEL_DIM), jnp.float32)) * ln_grad ** 2
    embed_mom1 = jax.random.normal(shared_keys[4], (VOCAB_SIZE, MODEL_DIM), jnp.float32) * embed_grad
    embed_mom2 = (0.5 + jax.random.uniform(shared_keys[5], (VOCAB_SIZE, MODEL_DIM), jnp.float32)) * embed_grad ** 2
    return {"hidden": hidden, "targets": targets, "loss_mask": loss_mask, "ln_params": ln_params, "out_embed": out_embed, "ln_mom1": ln_mom1, "ln_mom2": ln_mom2, "embed_mom1": embed_mom1, "embed_mom2": embed_mom2}


def layer_norm(hidden, ln_params):
    rows_f32 = hidden.astype(jnp.float32)
    row_mean = jnp.mean(rows_f32, axis=-1, keepdims=True)
    centered = rows_f32 - row_mean
    row_var = jnp.mean(centered * centered, axis=-1, keepdims=True)
    normed = centered * lax.rsqrt(row_var + LN_EPS)
    return normed * ln_params[0] + ln_params[1]


def adam_step(param_val, grad_val, m_old, v_old, decay_rate):
    m_new = BETA_ONE * m_old + (1.0 - BETA_ONE) * grad_val
    v_new = BETA_TWO * v_old + (1.0 - BETA_TWO) * grad_val * grad_val
    m_hat = m_new / (1.0 - BETA_ONE ** ADAM_STEP)
    v_hat = v_new / (1.0 - BETA_TWO ** ADAM_STEP)
    new_param = param_val - LEARN_RATE * (m_hat / (jnp.sqrt(v_hat) + ADAM_EPS) + decay_rate * param_val)
    return new_param, m_new, v_new


def block_logits(x_block, out_embed):
    return jnp.dot(x_block, out_embed.T, preferred_element_type=jnp.float32)


def reference(hidden, targets, loss_mask, ln_params, out_embed, ln_mom1, ln_mom2, embed_mom1, embed_mom2):
    x_norm, ln_vjp = jax.vjp(layer_norm, hidden, ln_params)
    x_bf = x_norm.astype(jnp.bfloat16)
    mask_f = loss_mask.astype(jnp.float32)
    valid_count = jnp.sum(mask_f)
    vocab_ids = jnp.arange(VOCAB_SIZE, dtype=jnp.int32)
    x_blocks = x_bf.reshape(NUM_BLOCKS, ROW_BLOCK, MODEL_DIM)
    tgt_blocks = targets.reshape(NUM_BLOCKS, ROW_BLOCK)
    scale_blocks = (mask_f / valid_count).reshape(NUM_BLOCKS, ROW_BLOCK)

    def forward_block(block_in):
        x_block, tgt_block = block_in
        logits = block_logits(x_block, out_embed)
        lse_block = jax.nn.logsumexp(logits, axis=-1)
        is_target = vocab_ids[None, :] == tgt_block[:, None]
        tgt_logit = jnp.sum(jnp.where(is_target, logits, 0.0), axis=-1)
        return lse_block, tgt_logit

    lse_blocks, tgt_logits = lax.map(forward_block, (x_blocks, tgt_blocks))
    token_loss = (lse_blocks.reshape(SEQ_LEN) - tgt_logits.reshape(SEQ_LEN)) * mask_f
    mean_loss = (jnp.sum(token_loss) / valid_count).reshape(1)

    def backward_block(d_embed, block_in):
        x_block, tgt_block, lse_block, scale_block = block_in
        logits = block_logits(x_block, out_embed)
        prob_vals = jnp.exp(logits - lse_block[:, None])
        is_target = (vocab_ids[None, :] == tgt_block[:, None]).astype(jnp.float32)
        d_logits = ((prob_vals - is_target) * scale_block[:, None]).astype(jnp.bfloat16)
        d_embed = d_embed + jnp.dot(d_logits.T, x_block, preferred_element_type=jnp.float32)
        d_x = jnp.dot(d_logits, out_embed, preferred_element_type=jnp.float32)
        return d_embed, d_x

    d_embed, d_x = lax.scan(backward_block, jnp.zeros((VOCAB_SIZE, MODEL_DIM), jnp.float32), (x_blocks, tgt_blocks, lse_blocks, scale_blocks))
    d_hidden, d_ln = ln_vjp(d_x.reshape(SEQ_LEN, MODEL_DIM))
    ln_new, ln_mom1_new, ln_mom2_new = adam_step(ln_params, d_ln, ln_mom1, ln_mom2, 0.0)
    embed_f, embed_mom1_new, embed_mom2_new = adam_step(out_embed.astype(jnp.float32), d_embed, embed_mom1, embed_mom2, WEIGHT_DECAY)
    return (token_loss, mean_loss, d_hidden, ln_new, ln_mom1_new, ln_mom2_new, embed_f.astype(jnp.bfloat16), embed_mom1_new, embed_mom2_new)
```

```python
import functools

import jax
import jax.numpy as jnp
from jax import lax
from jax.experimental import pallas as pl
from jax.experimental.pallas import tpu as pltpu
from jax.sharding import PartitionSpec as P

LN_EPS = 1e-5
BETA_ONE = 0.9
BETA_TWO = 0.95
ADAM_EPS = 1e-8
LEARN_RATE = 1e-3
WEIGHT_DECAY = 0.1
ADAM_STEP = 10

MESH = pl.DeviceIdType.MESH
VMEM_LIMIT = 64_000_000
NEG = -3.0e38
STAT_ROWS = 64
DOT_ROWS = 1056


def layer_norm(hidden, ln_params):
    rows_f32 = hidden.astype(jnp.float32)
    row_mean = jnp.mean(rows_f32, axis=-1, keepdims=True)
    centered = rows_f32 - row_mean
    row_var = jnp.mean(centered * centered, axis=-1, keepdims=True)
    normed = centered * lax.rsqrt(row_var + LN_EPS)
    return normed * ln_params[0:1] + ln_params[1:2]


def adam_step(param_val, grad_val, m_old, v_old, decay_rate):
    m_new = BETA_ONE * m_old + (1.0 - BETA_ONE) * grad_val
    v_new = BETA_TWO * v_old + (1.0 - BETA_TWO) * grad_val * grad_val
    m_hat = m_new / (1.0 - BETA_ONE ** ADAM_STEP)
    v_hat = v_new / (1.0 - BETA_TWO ** ADAM_STEP)
    new_param = param_val - LEARN_RATE * (m_hat / (jnp.sqrt(v_hat) + ADAM_EPS) + decay_rate * param_val)
    return new_param, m_new, v_new


def row_chunks(rows, size):
    return [(lo, min(size, rows - lo)) for lo in range(0, rows, size)]


def forward_kernel(n, tiles, hid, tm, lnp, e_hbm,
                   z_hbm, x_hbm, lse_o, scale_o, tgt_o, loss_o, mean_o,
                   x_all, x_send, tm_all, e_v, x_t, z_a, z_b, m_run, m_old, s_run, t_run, st_own, st_all,
                   e_sem, z_sem, xo_sem, sx_send, sx_recv, tm_send, tm_recv, st_send, st_recv):
    me = lax.axis_index("tp")
    chips = n // 2
    chip, core = me // 2, lax.rem(me, 2)
    sgn = 1 - 2 * core
    tok = hid.shape[0]
    vocab = e_hbm.shape[0]
    vt = vocab // tiles

    def dev(chip_idx, core_idx):
        return lax.rem(chip_idx + 2 * chips, chips) * 2 + core_idx

    e_copies = [pltpu.make_async_copy(e_hbm.at[pl.ds(t * vt, vt)], e_v.at[pl.ds(t * vt, vt)], e_sem.at[t]) for t in range(tiles)]
    for c in e_copies:
        c.start()

    barrier = pltpu.get_barrier_semaphore()
    for r in range(1, n):
        pl.semaphore_signal(barrier, inc=1, device_id={"tp": lax.rem(me + r, n)}, device_id_type=MESH)

    x_send[...] = layer_norm(hid[...], lnp[...]).astype(jnp.bfloat16)
    x_all[me] = x_send[...]
    tm_all[me] = tm[...]
    pl.semaphore_wait(barrier, n - 1)

    def xcopy(idx, src, slot, dst, recv):
        return pltpu.make_async_remote_copy(src_ref=src, dst_ref=x_all.at[slot], send_sem=sx_send.at[idx],
                                            recv_sem=sx_recv.at[recv], device_id={"tp": dst}, device_id_type=MESH)

    partner = dev(chip, 1 - core)
    ahead = dev(chip + sgn, core)
    behind = dev(chip - sgn, core)
    a1 = dev(chip - sgn, core)
    a2 = dev(chip + sgn, core)
    far = dev(chip + 2, core)
    s0 = xcopy(0, x_send, me, partner, 1)
    s1 = xcopy(1, x_send, me, ahead, 2)
    s2 = xcopy(2, x_send, me, behind, 4)
    s3 = xcopy(3, x_all.at[a1], a1, partner, 3)
    s4 = xcopy(4, x_all.at[a1], a1, ahead, 6)
    s5 = xcopy(5, x_all.at[a2], a2, partner, 5)
    s6 = xcopy(6, x_all.at[far], far, partner, 7)

    def tmcopy(r):
        peer = lax.rem(me + r, n)
        return pltpu.make_async_remote_copy(src_ref=tm, dst_ref=tm_all.at[me], send_sem=tm_send.at[r - 1],
                                            recv_sem=tm_recv.at[r - 1], device_id={"tp": peer}, device_id_type=MESH)

    tm_copies = [tmcopy(r) for r in range(1, n)]
    s0.start()
    for c in tm_copies:
        c.start()
    s1.start()
    for c in tm_copies:
        c.wait()

    def block_of(p):
        q = lax.rem(p, 2)
        h = p // 2
        own_core = core + q * sgn
        step = jnp.where(h == 0, 0, jnp.where(h == 1, -sgn, jnp.where(h == 2, sgn, 2)))
        flip = jnp.where(h == 3, 1, 1 - 2 * q)
        return dev(chip + step * flip, own_core)

    def z_copy(nn, buf):
        p, t = nn // tiles, lax.rem(nn, tiles)
        slot = lax.rem(nn, 2)
        return pltpu.make_async_copy(buf, z_hbm.at[block_of(p), pl.ds(pl.multiple_of(t * vt, 16), vt)], z_sem.at[slot])

    def x_out(p):
        b = block_of(p)
        return pltpu.make_async_copy(x_all.at[b], x_hbm.at[b], xo_sem.at[p])

    def reset():
        m_run[...] = jnp.full_like(m_run, NEG)
        m_old[...] = jnp.full_like(m_old, NEG)
        s_run[...] = jnp.zeros_like(s_run)
        t_run[...] = jnp.zeros_like(t_run)

    sub = lax.broadcasted_iota(jnp.int32, (8, tok), 0)

    def sums_begin(nn):
        p, t = nn // tiles, lax.rem(nn, tiles)
        want = tm_all[block_of(p)][0:1] - (me * vocab + t * vt) - sub
        m = m_run[...]
        return want, m, s_run[...] * jnp.exp(m_old[...] - m), t_run[...]

    def sums_rows(acc, buf, start, count):
        want, m, s, tgt = acc
        for lo, size in row_chunks(count, STAT_ROWS):
            z = buf[start + lo:start + lo + size, :].reshape(size // 8, 8, tok)
            s = s + jnp.sum(jnp.exp(z - m[None]), axis=0)
            rows = lax.broadcasted_iota(jnp.int32, z.shape, 0) * 8 + (start + lo)
            tgt = tgt + jnp.sum(jnp.where(want[None] == rows, z, 0.0), axis=0)
        return want, m, s, tgt

    def sums_end(acc):
        _, m_old[...], s_run[...], t_run[...] = acc

    def sums(nn, buf):
        sums_end(sums_rows(sums_begin(nn), buf, 0, vt))

    def st_copy(r, blk):
        peer = lax.rem(me + r, n)
        return pltpu.make_async_remote_copy(src_ref=st_own.at[blk], dst_ref=st_all.at[me, blk], send_sem=st_send.at[r - 1],
                                            recv_sem=st_recv.at[r - 1], device_id={"tp": peer}, device_id_type=MESH)

    def finish(p):
        b = block_of(p)
        m, s = m_run[...], s_run[...]
        m_all = jnp.max(m, axis=0, keepdims=True)
        s_sum = jnp.sum(s * jnp.exp(m - m_all), axis=0, keepdims=True)
        both = jnp.concatenate([m_all + jnp.log(s_sum), jnp.sum(t_run[...], axis=0, keepdims=True)], axis=0)
        st_own[b] = both
        st_all[me, b] = both

    def send_stats(p):
        b = block_of(p)
        for r in range(1, n):
            st_copy(r, b).start()

    reset()

    def step(nn, cur, prev):
        p, t = nn // tiles, lax.rem(nn, tiles)

        @pl.when(t == 0)
        def _():
            @pl.when(p == 1)
            def _():
                s0.wait_recv()

            @pl.when(p == 2)
            def _():
                s1.wait()
                s3.start()
                s2.start()

            @pl.when(p == 3)
            def _():
                s3.wait_recv()
                s4.start()

            @pl.when(p == 4)
            def _():
                s2.wait()
                s5.start()

            @pl.when(p == 5)
            def _():
                s5.wait_recv()

            @pl.when(p == 6)
            def _():
                s4.wait_recv()
                s6.start()

            @pl.when(p == 7)
            def _():
                s6.wait_recv()

            b = block_of(p)
            x_out(p).start()
            x_t[...] = x_all[b].T

        for tt in range(tiles):
            @pl.when(nn == tt)
            def _():
                e_copies[tt].wait()

        @pl.when(nn >= 2)
        def _():
            z_copy(nn - 2, cur).wait()

        top = jnp.full((8, tok), NEG, jnp.float32)
        acc = sums_begin(jnp.maximum(nn - 1, 0))
        for lo, size in row_chunks(vt, DOT_ROWS):
            z = jnp.dot(e_v[pl.ds(pl.multiple_of(t * vt + lo, 16), size), :], x_t[...], preferred_element_type=jnp.float32)
            cur[lo:lo + size, :] = z
            top = jnp.maximum(top, jnp.max(z.reshape(size // 8, 8, tok), axis=0))
            acc = sums_rows(acc, prev, lo, size)
        sums_end(acc)
        z_copy(nn, cur).start()

        @pl.when(t == 0)
        def _():
            @pl.when(nn > 0)
            def _():
                finish(p - 1)
            reset()

        m_run[...] = jnp.maximum(m_run[...], top)

        @pl.when((t == 1) & (p > 0))
        def _():
            send_stats(p - 1)

    def body(i, carry):
        step(2 * i, z_a, z_b)
        step(2 * i + 1, z_b, z_a)
        return carry

    total = n * tiles
    lax.fori_loop(0, total // 2, body, 0)
    sums(total - 1, z_b)
    finish(n - 1)
    z_copy(total - 2, z_a).wait()
    send_stats(n - 1)
    z_copy(total - 1, z_b).wait()
    for c in (s0, s2, s3, s4, s5, s6):
        pass
    s0.wait_send()
    s3.wait_send()
    s4.wait_send()
    s5.wait_send()
    s6.wait_send()
    for p in range(n):
        x_out(p).wait()

    for r in range(1, n):
        src = lax.rem(me + n - r, n)
        pltpu.make_async_remote_copy(src_ref=st_own, dst_ref=st_all.at[src], send_sem=st_send.at[r - 1],
                                     recv_sem=st_recv.at[r - 1], device_id={"tp": src}, device_id_type=MESH).wait()

    parts = [st_all[d] for d in range(n)]
    lses = [q[:, 0, :] for q in parts]
    top = functools.reduce(jnp.maximum, lses)
    lse = top + jnp.log(sum(jnp.exp(q - top) for q in lses))
    tgt_logit = sum(q[:, 1, :] for q in parts)
    tm_full = tm_all[...]
    mask = tm_full[:, 1, :].astype(jnp.float32)
    count = jnp.sum(mask)
    loss = (lse - tgt_logit) * mask
    lse_o[...] = lse
    scale_o[...] = mask / count
    tgt_o[...] = tm_full[:, 0, :] - me * vocab
    own = lax.broadcasted_iota(jnp.int32, loss.shape, 0) == me
    loss_o[...] = jnp.sum(jnp.where(own, loss, 0.0), axis=0, keepdims=True)
    mean_o[...] = jnp.full(mean_o.shape, jnp.sum(loss) / count, jnp.float32)


def forward(n, hidden, tm, ln_params, out_embed):
    tok, dim = hidden.shape
    vocab = out_embed.shape[0]
    tiles = 3
    vt = vocab // tiles
    vmem = pl.BlockSpec(memory_space=pltpu.VMEM)
    hbm = pl.BlockSpec(memory_space=pl.ANY)
    f32, bf16, i32 = jnp.float32, jnp.bfloat16, jnp.int32
    dma = pltpu.SemaphoreType.DMA
    return pl.pallas_call(
        functools.partial(forward_kernel, n, tiles),
        name="forward",
        out_shape=(
            jax.ShapeDtypeStruct((n, vocab, tok), f32),
            jax.ShapeDtypeStruct((n, tok, dim), bf16),
            jax.ShapeDtypeStruct((n, tok), f32),
            jax.ShapeDtypeStruct((n, tok), f32),
            jax.ShapeDtypeStruct((n, tok), i32),
            jax.ShapeDtypeStruct((1, tok), f32),
            jax.ShapeDtypeStruct((1, 128), f32),
        ),
        in_specs=[vmem, vmem, vmem, hbm],
        out_specs=(hbm, hbm, vmem, vmem, vmem, vmem, vmem),
        scratch_shapes=[
            pltpu.VMEM((n, tok, dim), bf16),
            pltpu.VMEM((tok, dim), bf16),
            pltpu.VMEM((n, 2, tok), i32),
            pltpu.VMEM((vocab, dim), bf16),
            pltpu.VMEM((dim, tok), bf16),
            pltpu.VMEM((vt, tok), f32),
            pltpu.VMEM((vt, tok), f32),
            pltpu.VMEM((8, tok), f32),
            pltpu.VMEM((8, tok), f32),
            pltpu.VMEM((8, tok), f32),
            pltpu.VMEM((8, tok), f32),
            pltpu.VMEM((n, 2, tok), f32),
            pltpu.VMEM((n, n, 2, tok), f32),
            dma((tiles,)), dma((2,)), dma((n,)),
            dma((7,)), dma((8,)), dma((n - 1,)), dma((n - 1,)), dma((n - 1,)), dma((n - 1,)),
        ],
        compiler_params=pltpu.CompilerParams(collective_id=0, has_side_effects=True, vmem_limit_bytes=VMEM_LIMIT),
        cost_estimate=pl.CostEstimate(flops=2 * n * tok * dim * vocab, bytes_accessed=4 * n * tok * vocab, transcendentals=n * tok * vocab),
    )(hidden, tm, ln_params, out_embed)


def dx_kernel(z, e, lse, scale, tgt, dz_o, dx_o, e_t):
    b, t = pl.program_id(0), pl.program_id(1)
    vt, tok = z.shape

    @pl.when(b == 0)
    def _():
        e_t[t] = e[...].T

    l, sc = lse[...], scale[...]
    want = tgt[...] - t * vt
    for lo, size in row_chunks(vt, 128):
        rows = lax.broadcasted_iota(jnp.int32, (size, tok), 0) + lo
        hot = jnp.where(rows == want, 1.0, 0.0)
        dz_o[lo:lo + size, :] = ((jnp.exp(z[lo:lo + size, :] - l) - hot) * sc).astype(jnp.bfloat16)
    part = jnp.dot(e_t[t], dz_o[...], preferred_element_type=jnp.float32)

    @pl.when(t == 0)
    def _():
        dx_o[...] = part

    @pl.when(t > 0)
    def _():
        dx_o[...] += part


def dz_dx(z, out_embed, lse, scale, tgt):
    n, vocab, tok = z.shape
    dim = out_embed.shape[1]
    tiles = 3
    vt = vocab // tiles
    f32, bf16 = jnp.float32, jnp.bfloat16
    row = pl.BlockSpec((None, 1, tok), lambda b, t: (b, 0, 0))
    return pl.pallas_call(
        dx_kernel,
        name="dz_dx",
        grid=(n, tiles),
        in_specs=[
            pl.BlockSpec((None, vt, tok), lambda b, t: (b, t, 0)),
            pl.BlockSpec((vt, dim), lambda b, t: (jnp.where(b == 0, t, tiles - 1), 0)),
            row, row, row,
        ],
        out_specs=(
            pl.BlockSpec((vt, tok), lambda b, t: (t, b)),
            pl.BlockSpec((None, dim, tok), lambda b, t: (b, 0, 0)),
        ),
        out_shape=(jax.ShapeDtypeStruct((vocab, n * tok), bf16), jax.ShapeDtypeStruct((n, dim, tok), f32)),
        scratch_shapes=[pltpu.VMEM((tiles, dim, vt), bf16)],
        compiler_params=pltpu.CompilerParams(vmem_limit_bytes=VMEM_LIMIT, dimension_semantics=("arbitrary", "arbitrary")),
        cost_estimate=pl.CostEstimate(flops=2 * n * tok * dim * vocab, bytes_accessed=6 * n * tok * vocab, transcendentals=n * tok * vocab),
    )(z, out_embed, lse.reshape(n, 1, tok), scale.reshape(n, 1, tok), tgt.reshape(n, 1, tok))


def update_kernel(dz, x, e, m, v, e_o, m_o, v_o, grad):
    i = pl.program_id(0)
    last = pl.num_programs(0) - 1

    def adam():
        g = grad[lax.rem(i + 1, 2)]
        new_e, m_o[...], v_o[...] = adam_step(e[...].astype(jnp.float32), g, m[...], v[...], WEIGHT_DECAY)
        e_o[...] = new_e.astype(jnp.bfloat16)

    @pl.when(i < last)
    def _():
        grad[lax.rem(i, 2)] = jnp.dot(dz[...], x[...], preferred_element_type=jnp.float32)
        adam()

    @pl.when(i == last)
    def _():
        adam()


def update(dz, x, out_embed, mom1, mom2):
    vocab, dim = out_embed.shape
    toks = x.shape[0]
    vt = 640
    steps = pl.cdiv(vocab, vt)
    f32, bf16 = jnp.float32, jnp.bfloat16
    late = pl.BlockSpec((vt, dim), lambda i: (jnp.maximum(i - 1, 0), 0))
    return pl.pallas_call(
        update_kernel,
        name="update",
        grid=(steps + 1,),
        in_specs=[
            pl.BlockSpec((vt, toks), lambda i: (jnp.minimum(i, steps - 1), 0)),
            pl.BlockSpec((toks, dim), lambda i: (0, 0)),
            late, late, late,
        ],
        out_specs=(late, late, late),
        out_shape=(jax.ShapeDtypeStruct((vocab, dim), bf16), jax.ShapeDtypeStruct((vocab, dim), f32), jax.ShapeDtypeStruct((vocab, dim), f32)),
        scratch_shapes=[pltpu.VMEM((2, vt, dim), f32)],
        compiler_params=pltpu.CompilerParams(vmem_limit_bytes=VMEM_LIMIT, dimension_semantics=("arbitrary",)),
        cost_estimate=pl.CostEstimate(flops=2 * toks * dim * vocab, bytes_accessed=2 * toks * vocab + 20 * vocab * dim, transcendentals=2 * vocab * dim),
    )(dz, x, out_embed, mom1, mom2)


def solution(mesh):
    n = mesh.shape["tp"]
    row_spec = P(("dp", "tp"), None)
    tok_spec = P(("dp", "tp"))
    vocab_spec = P("tp", None)
    repl_spec = P()
    part_spec = P("dp", None)

    def device_step(hidden, targets, loss_mask, ln_params, out_embed, ln_mom1, ln_mom2, embed_mom1, embed_mom2):
        tok, dim = hidden.shape
        tm = jnp.stack([targets, loss_mask])
        z, x_full, lse, scale, tgt, loss, mean = forward(n, hidden, tm, ln_params, out_embed)
        dz, dx = dz_dx(z, out_embed, lse, scale, tgt)
        d_x_t = lax.psum_scatter(dx, "tp", scatter_dimension=0, tiled=False)
        embed_new, embed_mom1_new, embed_mom2_new = update(dz, x_full.reshape(n * tok, dim), out_embed, embed_mom1, embed_mom2)
        _, ln_vjp = jax.vjp(layer_norm, hidden, ln_params)
        d_hidden, d_ln = ln_vjp(d_x_t.T)
        d_ln = lax.psum(d_ln, "tp")
        ln_new, ln_mom1_new, ln_mom2_new = adam_step(ln_params, d_ln, ln_mom1, ln_mom2, 0.0)
        return (loss.reshape(tok), mean[0, :1], d_hidden, ln_new, ln_mom1_new, ln_mom2_new, embed_new, embed_mom1_new, embed_mom2_new)

    return jax.shard_map(device_step, mesh=mesh, in_specs=(row_spec, tok_spec, tok_spec, repl_spec, vocab_spec, repl_spec, repl_spec, vocab_spec, vocab_spec), out_specs=(tok_spec, P("dp"), row_spec, part_spec, part_spec, part_spec, row_spec, row_spec, row_spec), check_vma=False)
```

```python
import functools

import jax
import jax.numpy as jnp
from jax import lax
from jax.experimental import pallas as pl
from jax.experimental.pallas import tpu as pltpu
from jax.sharding import PartitionSpec as P

LN_EPS = 1e-5
BETA_ONE = 0.9
BETA_TWO = 0.95
ADAM_EPS = 1e-8
LEARN_RATE = 1e-3
WEIGHT_DECAY = 0.1
ADAM_STEP = 10

MESH = pl.DeviceIdType.MESH
VMEM_LIMIT = 64_000_000
NEG = -3.0e38
STAT_ROWS = 64
ADAM_ROWS = 64
DOT_ROWS = 1056


def layer_norm(hidden, ln_params):
    rows_f32 = hidden.astype(jnp.float32)
    row_mean = jnp.mean(rows_f32, axis=-1, keepdims=True)
    centered = rows_f32 - row_mean
    row_var = jnp.mean(centered * centered, axis=-1, keepdims=True)
    normed = centered * lax.rsqrt(row_var + LN_EPS)
    return normed * ln_params[0:1] + ln_params[1:2]


def adam_step(param_val, grad_val, m_old, v_old, decay_rate):
    m_new = BETA_ONE * m_old + (1.0 - BETA_ONE) * grad_val
    v_new = BETA_TWO * v_old + (1.0 - BETA_TWO) * grad_val * grad_val
    m_hat = m_new / (1.0 - BETA_ONE ** ADAM_STEP)
    v_hat = v_new / (1.0 - BETA_TWO ** ADAM_STEP)
    new_param = param_val - LEARN_RATE * (m_hat / (jnp.sqrt(v_hat) + ADAM_EPS) + decay_rate * param_val)
    return new_param, m_new, v_new


def row_chunks(rows, size):
    return [(lo, min(size, rows - lo)) for lo in range(0, rows, size)]


def forward_kernel(n, tiles, hid, tm, lnp, e_hbm,
                   z_hbm, x_hbm, lse_o, scale_o, tgt_o, loss_o, mean_o,
                   x_all, x_send, tm_all, e_v, x_t, z_a, z_b, m_run, m_old, s_run, t_run, st_own, st_all,
                   e_sem, z_sem, xo_sem, sx_send, sx_recv, tm_send, tm_recv, st_send, st_recv):
    me = lax.axis_index("tp")
    chips = n // 2
    chip, core = me // 2, lax.rem(me, 2)
    sgn = 1 - 2 * core
    tok = hid.shape[0]
    vocab = e_hbm.shape[0]
    vt = vocab // tiles

    def dev(chip_idx, core_idx):
        return lax.rem(chip_idx + 2 * chips, chips) * 2 + core_idx

    e_copies = [pltpu.make_async_copy(e_hbm.at[pl.ds(t * vt, vt)], e_v.at[pl.ds(t * vt, vt)], e_sem.at[t]) for t in range(tiles)]
    for c in e_copies:
        c.start()

    barrier = pltpu.get_barrier_semaphore()
    for r in range(1, n):
        pl.semaphore_signal(barrier, inc=1, device_id={"tp": lax.rem(me + r, n)}, device_id_type=MESH)

    x_send[...] = layer_norm(hid[...], lnp[...]).astype(jnp.bfloat16)
    x_all[me] = x_send[...]
    tm_all[me] = tm[...]
    pl.semaphore_wait(barrier, n - 1)

    def xcopy(idx, src, slot, dst, recv):
        return pltpu.make_async_remote_copy(src_ref=src, dst_ref=x_all.at[slot], send_sem=sx_send.at[idx],
                                            recv_sem=sx_recv.at[recv], device_id={"tp": dst}, device_id_type=MESH)

    partner = dev(chip, 1 - core)
    ahead = dev(chip + sgn, core)
    behind = dev(chip - sgn, core)
    a1 = dev(chip - sgn, core)
    a2 = dev(chip + sgn, core)
    far = dev(chip + 2, core)
    s0 = xcopy(0, x_send, me, partner, 1)
    s1 = xcopy(1, x_send, me, ahead, 2)
    s2 = xcopy(2, x_send, me, behind, 4)
    s3 = xcopy(3, x_all.at[a1], a1, partner, 3)
    s4 = xcopy(4, x_all.at[a1], a1, ahead, 6)
    s5 = xcopy(5, x_all.at[a2], a2, partner, 5)
    s6 = xcopy(6, x_all.at[far], far, partner, 7)

    def tmcopy(r):
        peer = lax.rem(me + r, n)
        return pltpu.make_async_remote_copy(src_ref=tm, dst_ref=tm_all.at[me], send_sem=tm_send.at[r - 1],
                                            recv_sem=tm_recv.at[r - 1], device_id={"tp": peer}, device_id_type=MESH)

    tm_copies = [tmcopy(r) for r in range(1, n)]
    s0.start()
    for c in tm_copies:
        c.start()
    s1.start()
    for c in tm_copies:
        c.wait()

    def block_of(p):
        q = lax.rem(p, 2)
        h = p // 2
        own_core = core + q * sgn
        step = jnp.where(h == 0, 0, jnp.where(h == 1, -sgn, jnp.where(h == 2, sgn, 2)))
        flip = jnp.where(h == 3, 1, 1 - 2 * q)
        return dev(chip + step * flip, own_core)

    def z_copy(nn, buf):
        p, t = nn // tiles, lax.rem(nn, tiles)
        slot = lax.rem(nn, 2)
        return pltpu.make_async_copy(buf, z_hbm.at[block_of(p), pl.ds(pl.multiple_of(t * vt, 16), vt)], z_sem.at[slot])

    def x_out(p):
        b = block_of(p)
        return pltpu.make_async_copy(x_all.at[b], x_hbm.at[b], xo_sem.at[p])

    def reset():
        m_run[...] = jnp.full_like(m_run, NEG)
        m_old[...] = jnp.full_like(m_old, NEG)
        s_run[...] = jnp.zeros_like(s_run)
        t_run[...] = jnp.zeros_like(t_run)

    sub = lax.broadcasted_iota(jnp.int32, (8, tok), 0)

    def sums_begin(nn):
        p, t = nn // tiles, lax.rem(nn, tiles)
        want = tm_all[block_of(p)][0:1] - (me * vocab + t * vt) - sub
        m = m_run[...]
        return want, m, s_run[...] * jnp.exp(m_old[...] - m), t_run[...]

    def sums_rows(acc, buf, start, count):
        want, m, s, tgt = acc
        for lo, size in row_chunks(count, STAT_ROWS):
            z = buf[start + lo:start + lo + size, :].reshape(size // 8, 8, tok)
            s = s + jnp.sum(jnp.exp(z - m[None]), axis=0)
            rows = lax.broadcasted_iota(jnp.int32, z.shape, 0) * 8 + (start + lo)
            tgt = tgt + jnp.sum(jnp.where(want[None] == rows, z, 0.0), axis=0)
        return want, m, s, tgt

    def sums_end(acc):
        _, m_old[...], s_run[...], t_run[...] = acc

    def sums(nn, buf):
        sums_end(sums_rows(sums_begin(nn), buf, 0, vt))

    def st_copy(r, blk):
        peer = lax.rem(me + r, n)
        return pltpu.make_async_remote_copy(src_ref=st_own.at[blk], dst_ref=st_all.at[me, blk], send_sem=st_send.at[r - 1],
                                            recv_sem=st_recv.at[r - 1], device_id={"tp": peer}, device_id_type=MESH)

    def finish(p):
        b = block_of(p)
        m, s = m_run[...], s_run[...]
        m_all = jnp.max(m, axis=0, keepdims=True)
        s_sum = jnp.sum(s * jnp.exp(m - m_all), axis=0, keepdims=True)
        both = jnp.concatenate([m_all + jnp.log(s_sum), jnp.sum(t_run[...], axis=0, keepdims=True)], axis=0)
        st_own[b] = both
        st_all[me, b] = both

    def send_stats(p):
        b = block_of(p)
        for r in range(1, n):
            st_copy(r, b).start()

    reset()

    def step(nn, cur, prev):
        p, t = nn // tiles, lax.rem(nn, tiles)

        @pl.when(t == 0)
        def _():
            @pl.when(p == 1)
            def _():
                s0.wait_recv()

            @pl.when(p == 2)
            def _():
                s1.wait()
                s3.start()
                s2.start()

            @pl.when(p == 3)
            def _():
                s3.wait_recv()
                s4.start()

            @pl.when(p == 4)
            def _():
                s2.wait()
                s5.start()

            @pl.when(p == 5)
            def _():
                s5.wait_recv()

            @pl.when(p == 6)
            def _():
                s4.wait_recv()
                s6.start()

            @pl.when(p == 7)
            def _():
                s6.wait_recv()

            b = block_of(p)
            x_out(p).start()
            x_t[...] = x_all[b].T

        for tt in range(tiles):
            @pl.when(nn == tt)
            def _():
                e_copies[tt].wait()

        @pl.when(nn >= 2)
        def _():
            z_copy(nn - 2, cur).wait()

        top = jnp.full((8, tok), NEG, jnp.float32)
        acc = sums_begin(jnp.maximum(nn - 1, 0))
        for lo, size in row_chunks(vt, DOT_ROWS):
            z = jnp.dot(e_v[pl.ds(pl.multiple_of(t * vt + lo, 16), size), :], x_t[...], preferred_element_type=jnp.float32)
            cur[lo:lo + size, :] = z
            top = jnp.maximum(top, jnp.max(z.reshape(size // 8, 8, tok), axis=0))
            acc = sums_rows(acc, prev, lo, size)
        sums_end(acc)
        z_copy(nn, cur).start()

        @pl.when(t == 0)
        def _():
            @pl.when(nn > 0)
            def _():
                finish(p - 1)
            reset()

        m_run[...] = jnp.maximum(m_run[...], top)

        @pl.when((t == 1) & (p > 0))
        def _():
            send_stats(p - 1)

    def body(i, carry):
        step(2 * i, z_a, z_b)
        step(2 * i + 1, z_b, z_a)
        return carry

    total = n * tiles
    lax.fori_loop(0, total // 2, body, 0)
    sums(total - 1, z_b)
    finish(n - 1)
    z_copy(total - 2, z_a).wait()
    send_stats(n - 1)
    z_copy(total - 1, z_b).wait()
    s0.wait_send()
    s3.wait_send()
    s4.wait_send()
    s5.wait_send()
    s6.wait_send()
    for p in range(n):
        x_out(p).wait()

    for r in range(1, n):
        src = lax.rem(me + n - r, n)
        pltpu.make_async_remote_copy(src_ref=st_own, dst_ref=st_all.at[src], send_sem=st_send.at[r - 1],
                                     recv_sem=st_recv.at[r - 1], device_id={"tp": src}, device_id_type=MESH).wait()

    parts = [st_all[d] for d in range(n)]
    lses = [q[:, 0, :] for q in parts]
    top = functools.reduce(jnp.maximum, lses)
    lse = top + jnp.log(sum(jnp.exp(q - top) for q in lses))
    tgt_logit = sum(q[:, 1, :] for q in parts)
    tm_full = tm_all[...]
    mask = tm_full[:, 1, :].astype(jnp.float32)
    count = jnp.sum(mask)
    loss = (lse - tgt_logit) * mask
    for d in range(n):
        lse_o[d] = lse[d:d + 1]
        scale_o[d] = mask[d:d + 1] / count
        tgt_o[d] = tm_full[d, 0:1, :] - me * vocab
    own = lax.broadcasted_iota(jnp.int32, loss.shape, 0) == me
    loss_o[...] = jnp.sum(jnp.where(own, loss, 0.0), axis=0, keepdims=True)
    mean_o[...] = jnp.full(mean_o.shape, jnp.sum(loss) / count, jnp.float32)


def forward(n, hidden, tm, ln_params, out_embed):
    tok, dim = hidden.shape
    vocab = out_embed.shape[0]
    tiles = 3
    vt = vocab // tiles
    vmem = pl.BlockSpec(memory_space=pltpu.VMEM)
    hbm = pl.BlockSpec(memory_space=pl.ANY)
    f32, bf16, i32 = jnp.float32, jnp.bfloat16, jnp.int32
    dma = pltpu.SemaphoreType.DMA
    return pl.pallas_call(
        functools.partial(forward_kernel, n, tiles),
        name="forward",
        out_shape=(
            jax.ShapeDtypeStruct((n, vocab, tok), f32),
            jax.ShapeDtypeStruct((n, tok, dim), bf16),
            jax.ShapeDtypeStruct((n, 1, tok), f32),
            jax.ShapeDtypeStruct((n, 1, tok), f32),
            jax.ShapeDtypeStruct((n, 1, tok), i32),
            jax.ShapeDtypeStruct((1, tok), f32),
            jax.ShapeDtypeStruct((1, 128), f32),
        ),
        in_specs=[vmem, vmem, vmem, hbm],
        out_specs=(hbm, hbm, vmem, vmem, vmem, vmem, vmem),
        scratch_shapes=[
            pltpu.VMEM((n, tok, dim), bf16),
            pltpu.VMEM((tok, dim), bf16),
            pltpu.VMEM((n, 2, tok), i32),
            pltpu.VMEM((vocab, dim), bf16),
            pltpu.VMEM((dim, tok), bf16),
            pltpu.VMEM((vt, tok), f32),
            pltpu.VMEM((vt, tok), f32),
            pltpu.VMEM((8, tok), f32),
            pltpu.VMEM((8, tok), f32),
            pltpu.VMEM((8, tok), f32),
            pltpu.VMEM((8, tok), f32),
            pltpu.VMEM((n, 2, tok), f32),
            pltpu.VMEM((n, n, 2, tok), f32),
            dma((tiles,)), dma((2,)), dma((n,)),
            dma((7,)), dma((8,)), dma((n - 1,)), dma((n - 1,)), dma((n - 1,)), dma((n - 1,)),
        ],
        compiler_params=pltpu.CompilerParams(collective_id=0, has_side_effects=True, vmem_limit_bytes=VMEM_LIMIT),
        cost_estimate=pl.CostEstimate(flops=2 * n * tok * dim * vocab, bytes_accessed=4 * n * tok * vocab, transcendentals=n * tok * vocab),
    )(hidden, tm, ln_params, out_embed)


def backward_kernel(n, tiles, hid, lnp, lnm1, lnm2, lse, scale, tgt, z_hbm, e_hbm,
                    dz_hbm, dh_o, lnp_o, lnm1_o, lnm2_o,
                    z_0, z_1, z_2, dz_0, dz_1, dz_2, e_in, e_t, acc, to_pair, from_pair, to_ring, from_ring, d_ln,
                    z_sem, dz_sem, e_sem, pair_send, pair_recv, ring_send, ring_recv, ln_send, ln_recv):
    me = lax.axis_index("tp")
    chips = n // 2
    chip, core = me // 2, lax.rem(me, 2)
    sgn = 1 - 2 * core
    vt, tok = z_0.shape
    z_bufs, dz_bufs = (z_0, z_1, z_2), (dz_0, dz_1, dz_2)

    def dev(chip_idx, core_idx):
        return lax.rem(chip_idx + 2 * chips, chips) * 2 + core_idx

    partner = dev(chip, 1 - core)
    ahead = dev(chip + sgn, core)

    def block_of(q):
        s, own = q // 2, lax.rem(q, 2)
        return dev(chip + sgn * (1 + s) * (1 - 2 * own), jnp.where(own == 1, core, 1 - core))

    def z_copy(q, t):
        return pltpu.make_async_copy(z_hbm.at[block_of(q), pl.ds(t * vt, vt)], z_bufs[t], z_sem.at[t])

    def dz_copy(q, t):
        cols = pl.ds(pl.multiple_of(block_of(q) * tok, tok), tok)
        return pltpu.make_async_copy(dz_bufs[t], dz_hbm.at[pl.ds(t * vt, vt), cols], dz_sem.at[t])

    e_copies = [pltpu.make_async_copy(e_hbm.at[pl.ds(t * vt, vt)], e_in.at[pl.ds(t * vt, vt)], e_sem.at[t]) for t in range(tiles)]
    for t in range(tiles):
        e_copies[t].start()
        z_copy(0, t).start()

    barrier = pltpu.get_barrier_semaphore()
    for r in range(1, n):
        pl.semaphore_signal(barrier, inc=1, device_id={"tp": lax.rem(me + r, n)}, device_id_type=MESH)
    pl.semaphore_wait(barrier, n - 1)

    def pair_copy(s):
        return pltpu.make_async_remote_copy(src_ref=to_pair.at[lax.rem(s, 2)], dst_ref=from_pair.at[s], send_sem=pair_send.at[s],
                                            recv_sem=pair_recv.at[s], device_id={"tp": partner}, device_id_type=MESH)

    def ring_copy(s):
        return pltpu.make_async_remote_copy(src_ref=to_ring.at[lax.rem(s, 2)], dst_ref=from_ring.at[s], send_sem=ring_send.at[s],
                                            recv_sem=ring_recv.at[s], device_id={"tp": ahead}, device_id_type=MESH)

    last_step = chips - 1

    def tile_step(q, t, l, sc, want):
        z, dz = z_bufs[t], dz_bufs[t]

        @pl.when(q == 0)
        def _():
            e_copies[t].wait()
            e_t[t] = e_in[t * vt:(t + 1) * vt, :].T

        @pl.when(q > 0)
        def _():
            dz_copy(q - 1, t).wait()

        z_copy(q, t).wait()
        for lo, size in row_chunks(vt, 128):
            rows = lax.broadcasted_iota(jnp.int32, (size, tok), 0) + (t * vt + lo)
            hot = jnp.where(rows == want, 1.0, 0.0)
            dz[lo:lo + size, :] = ((jnp.exp(z[lo:lo + size, :] - l) - hot) * sc).astype(jnp.bfloat16)
        part = jnp.dot(e_t[t], dz[...], preferred_element_type=jnp.float32)
        if t == 0:
            acc[...] = part
        else:
            acc[...] += part
        dz_copy(q, t).start()

        @pl.when(q < n - 1)
        def _():
            z_copy(q + 1, t).start()

    def body(q, carry):
        b = block_of(q)
        l, sc, want = lse[b], scale[b], tgt[b]
        for t in range(tiles):
            tile_step(q, t, l, sc, want)
        s = q // 2

        @pl.when(lax.rem(q, 2) == 0)
        def _():
            @pl.when(s >= 2)
            def _():
                pair_copy(s - 2).wait_send()
            to_pair[lax.rem(s, 2)] = acc[...]
            pair_copy(s).start()

        @pl.when(lax.rem(q, 2) == 1)
        def _():
            pair_copy(s).wait_recv()
            acc[...] += from_pair[s]

            @pl.when(s > 0)
            def _():
                ring_copy(s - 1).wait_recv()
                acc[...] += from_ring[s - 1]

            @pl.when(s < last_step)
            def _():
                @pl.when(s >= 2)
                def _():
                    ring_copy(s - 2).wait_send()
                to_ring[lax.rem(s, 2)] = acc[...]
                ring_copy(s).start()

        return carry

    lax.fori_loop(0, n, body, 0)
    for s in (last_step - 1, last_step):
        pair_copy(s).wait_send()
    for s in range(max(last_step - 2, 0), last_step):
        ring_copy(s).wait_send()
    for t in range(tiles):
        dz_copy(n - 1, t).wait()

    d_x = acc[...].T
    rows = hid[...].astype(jnp.float32)
    centered = rows - jnp.mean(rows, axis=-1, keepdims=True)
    rstd = lax.rsqrt(jnp.mean(centered * centered, axis=-1, keepdims=True) + LN_EPS)
    normed = centered * rstd
    gain = lnp[0:1, :]
    d_ln[me] = jnp.concatenate([jnp.sum(d_x * normed, axis=0, keepdims=True), jnp.sum(d_x, axis=0, keepdims=True)], axis=0)

    def ln_copy(r, slot, peer):
        return pltpu.make_async_remote_copy(src_ref=d_ln.at[slot], dst_ref=d_ln.at[slot], send_sem=ln_send.at[r - 1],
                                            recv_sem=ln_recv.at[r - 1], device_id={"tp": peer}, device_id_type=MESH)

    d_normed = d_x * gain
    proj = jnp.mean(d_normed * normed, axis=-1, keepdims=True)
    dh_o[...] = (rstd * (d_normed - jnp.mean(d_normed, axis=-1, keepdims=True) - normed * proj)).astype(jnp.bfloat16)
    for r in range(1, n):
        ln_copy(r, me, lax.rem(me + r, n)).start()
    for r in range(1, n):
        src = lax.rem(me + n - r, n)
        ln_copy(r, src, src).wait()
    grad = d_ln[0]
    for d in range(1, n):
        grad = grad + d_ln[d]
    lnp_o[...], lnm1_o[...], lnm2_o[...] = adam_step(lnp[...], grad, lnm1[...], lnm2[...], 0.0)


def backward(n, hidden, ln_params, ln_mom1, ln_mom2, lse, scale, tgt, z, out_embed):
    tok, dim = hidden.shape
    vocab = out_embed.shape[0]
    tiles = 3
    vt = vocab // tiles
    chips = n // 2
    f32, bf16 = jnp.float32, jnp.bfloat16
    vmem = pl.BlockSpec(memory_space=pltpu.VMEM)
    hbm = pl.BlockSpec(memory_space=pl.ANY)
    dma = pltpu.SemaphoreType.DMA
    return pl.pallas_call(
        functools.partial(backward_kernel, n, tiles),
        name="backward",
        out_shape=(
            jax.ShapeDtypeStruct((vocab, n * tok), bf16),
            jax.ShapeDtypeStruct((tok, dim), bf16),
            jax.ShapeDtypeStruct((2, dim), f32),
            jax.ShapeDtypeStruct((2, dim), f32),
            jax.ShapeDtypeStruct((2, dim), f32),
        ),
        in_specs=[vmem] * 7 + [hbm, hbm],
        out_specs=(hbm, vmem, vmem, vmem, vmem),
        scratch_shapes=[pltpu.VMEM((vt, tok), f32)] * 3 + [pltpu.VMEM((vt, tok), bf16)] * 3 + [
            pltpu.VMEM((vocab, dim), bf16),
            pltpu.VMEM((tiles, dim, vt), bf16),
            pltpu.VMEM((dim, tok), f32),
            pltpu.VMEM((2, dim, tok), f32),
            pltpu.VMEM((chips, dim, tok), f32),
            pltpu.VMEM((2, dim, tok), f32),
            pltpu.VMEM((chips - 1, dim, tok), f32),
            pltpu.VMEM((n, 2, dim), f32),
            dma((tiles,)), dma((tiles,)), dma((tiles,)),
            dma((chips,)), dma((chips,)), dma((chips - 1,)), dma((chips - 1,)), dma((n - 1,)), dma((n - 1,)),
        ],
        compiler_params=pltpu.CompilerParams(collective_id=1, has_side_effects=True, vmem_limit_bytes=66_000_000),
        cost_estimate=pl.CostEstimate(flops=2 * n * tok * dim * vocab, bytes_accessed=6 * n * tok * vocab, transcendentals=n * tok * vocab),
    )(hidden, ln_params, ln_mom1, ln_mom2, lse, scale, tgt, z, out_embed)


def update_kernel(steps, dz, x, e, m, v, e_o, m_o, v_o, grad_a, grad_b):
    i = pl.program_id(0)

    def adam(grad):
        for lo, size in row_chunks(grad.shape[0], ADAM_ROWS):
            part = slice(lo, lo + size)
            new_e, m_o[part, :], v_o[part, :] = adam_step(e[part, :].astype(jnp.float32), grad[part, :], m[part, :], v[part, :], WEIGHT_DECAY)
            e_o[part, :] = new_e.astype(jnp.bfloat16)

    def both(new, old):
        adam(old)
        new[...] = jnp.dot(dz[...], x[...], preferred_element_type=jnp.float32)

    @pl.when((i < steps) & (lax.rem(i, 2) == 0))
    def _():
        both(grad_a, grad_b)

    @pl.when((i < steps) & (lax.rem(i, 2) == 1))
    def _():
        both(grad_b, grad_a)

    @pl.when(i == steps)
    def _():
        adam((grad_a, grad_b)[(steps - 1) % 2])


def update(dz, x, out_embed, mom1, mom2):
    vocab, dim = out_embed.shape
    toks = x.shape[0]
    vt = 640
    steps = pl.cdiv(vocab, vt)
    f32, bf16 = jnp.float32, jnp.bfloat16
    late = pl.BlockSpec((vt, dim), lambda i: (jnp.maximum(i - 1, 0), 0))
    return pl.pallas_call(
        functools.partial(update_kernel, steps),
        name="update",
        grid=(steps + 1,),
        in_specs=[
            pl.BlockSpec((vt, toks), lambda i: (jnp.minimum(i, steps - 1), 0)),
            pl.BlockSpec((toks, dim), lambda i: (0, 0)),
            late, late, late,
        ],
        out_specs=(late, late, late),
        out_shape=(jax.ShapeDtypeStruct((vocab, dim), bf16), jax.ShapeDtypeStruct((vocab, dim), f32), jax.ShapeDtypeStruct((vocab, dim), f32)),
        scratch_shapes=[pltpu.VMEM((vt, dim), f32), pltpu.VMEM((vt, dim), f32)],
        compiler_params=pltpu.CompilerParams(vmem_limit_bytes=VMEM_LIMIT, dimension_semantics=("arbitrary",)),
        cost_estimate=pl.CostEstimate(flops=2 * toks * dim * vocab, bytes_accessed=2 * toks * vocab + 20 * vocab * dim, transcendentals=2 * vocab * dim),
    )(dz, x, out_embed, mom1, mom2)


def solution(mesh):
    n = mesh.shape["tp"]
    row_spec = P(("dp", "tp"), None)
    tok_spec = P(("dp", "tp"))
    vocab_spec = P("tp", None)
    repl_spec = P()
    part_spec = P("dp", None)

    def device_step(hidden, targets, loss_mask, ln_params, out_embed, ln_mom1, ln_mom2, embed_mom1, embed_mom2):
        tok, dim = hidden.shape
        tm = jnp.stack([targets, loss_mask])
        z, x_full, lse, scale, tgt, loss, mean = forward(n, hidden, tm, ln_params, out_embed)
        dz, d_hidden, ln_new, ln_mom1_new, ln_mom2_new = backward(n, hidden, ln_params, ln_mom1, ln_mom2, lse, scale, tgt, z, out_embed)
        embed_new, embed_mom1_new, embed_mom2_new = update(dz, x_full.reshape(n * tok, dim), out_embed, embed_mom1, embed_mom2)
        return (loss.reshape(tok), mean[0, :1], d_hidden, ln_new, ln_mom1_new, ln_mom2_new, embed_new, embed_mom1_new, embed_mom2_new)

    return jax.shard_map(device_step, mesh=mesh, in_specs=(row_spec, tok_spec, tok_spec, repl_spec, vocab_spec, repl_spec, repl_spec, vocab_spec, vocab_spec), out_specs=(tok_spec, P("dp"), row_spec, part_spec, part_spec, part_spec, row_spec, row_spec, row_spec), check_vma=False)
```

```python
import functools

import jax
import jax.numpy as jnp
from jax import lax
from jax.experimental import pallas as pl
from jax.experimental.pallas import tpu as pltpu
from jax.sharding import PartitionSpec as P

LN_EPS = 1e-5
BETA_ONE = 0.9
BETA_TWO = 0.95
ADAM_EPS = 1e-8
LEARN_RATE = 1e-3
WEIGHT_DECAY = 0.1
ADAM_STEP = 10

MESH = pl.DeviceIdType.MESH
VMEM_LIMIT = 64_000_000
NEG = -3.0e38
STAT_ROWS = 64
ADAM_ROWS = 16
DZ_ROWS = 64
DOT_ROWS = 1056


def layer_norm(hidden, ln_params):
    rows_f32 = hidden.astype(jnp.float32)
    row_mean = jnp.mean(rows_f32, axis=-1, keepdims=True)
    centered = rows_f32 - row_mean
    row_var = jnp.mean(centered * centered, axis=-1, keepdims=True)
    normed = centered * lax.rsqrt(row_var + LN_EPS)
    return normed * ln_params[0:1] + ln_params[1:2]


def adam_step(param_val, grad_val, m_old, v_old, decay_rate):
    m_new = BETA_ONE * m_old + (1.0 - BETA_ONE) * grad_val
    v_new = BETA_TWO * v_old + (1.0 - BETA_TWO) * grad_val * grad_val
    m_step = m_new * (LEARN_RATE / (1.0 - BETA_ONE ** ADAM_STEP))
    v_hat = v_new * (1.0 / (1.0 - BETA_TWO ** ADAM_STEP))
    new_param = (1.0 - LEARN_RATE * decay_rate) * param_val - m_step / (jnp.sqrt(v_hat) + ADAM_EPS)
    return new_param, m_new, v_new


def row_chunks(rows, size):
    return [(lo, min(size, rows - lo)) for lo in range(0, rows, size)]


def forward_kernel(n, tiles, hid, tm, lnp, e_hbm,
                   z_hbm, x_hbm, lse_o, scale_o, tgt_o, loss_o, mean_o,
                   x_all, x_send, tm_all, e_v, x_t, z_a, z_b, m_run, m_old, s_run, t_run, st_own, st_all,
                   e_sem, z_sem, xo_sem, sx_send, sx_recv, tm_send, tm_recv, st_send, st_recv):
    me = lax.axis_index("tp")
    chips = n // 2
    chip, core = me // 2, lax.rem(me, 2)
    sgn = 1 - 2 * core
    tok = hid.shape[0]
    vocab = e_hbm.shape[0]
    vt = vocab // tiles

    def dev(chip_idx, core_idx):
        return lax.rem(chip_idx + 2 * chips, chips) * 2 + core_idx

    e_copies = [pltpu.make_async_copy(e_hbm.at[pl.ds(t * vt, vt)], e_v.at[pl.ds(t * vt, vt)], e_sem.at[t]) for t in range(tiles)]
    for c in e_copies:
        c.start()

    barrier = pltpu.get_barrier_semaphore()
    for r in range(1, n):
        pl.semaphore_signal(barrier, inc=1, device_id={"tp": lax.rem(me + r, n)}, device_id_type=MESH)

    x_send[...] = layer_norm(hid[...], lnp[...]).astype(jnp.bfloat16)
    x_all[me] = x_send[...]
    tm_all[me] = tm[...]
    pl.semaphore_wait(barrier, n - 1)

    def xcopy(idx, src, slot, dst, recv):
        return pltpu.make_async_remote_copy(src_ref=src, dst_ref=x_all.at[slot], send_sem=sx_send.at[idx],
                                            recv_sem=sx_recv.at[recv], device_id={"tp": dst}, device_id_type=MESH)

    partner = dev(chip, 1 - core)
    ahead = dev(chip + sgn, core)
    behind = dev(chip - sgn, core)
    a1 = dev(chip - sgn, core)
    a2 = dev(chip + sgn, core)
    far = dev(chip + 2, core)
    s0 = xcopy(0, x_send, me, partner, 1)
    s1 = xcopy(1, x_send, me, ahead, 2)
    s2 = xcopy(2, x_send, me, behind, 4)
    s3 = xcopy(3, x_all.at[a1], a1, partner, 3)
    s4 = xcopy(4, x_all.at[a1], a1, ahead, 6)
    s5 = xcopy(5, x_all.at[a2], a2, partner, 5)
    s6 = xcopy(6, x_all.at[far], far, partner, 7)

    def tmcopy(r):
        peer = lax.rem(me + r, n)
        return pltpu.make_async_remote_copy(src_ref=tm, dst_ref=tm_all.at[me], send_sem=tm_send.at[r - 1],
                                            recv_sem=tm_recv.at[r - 1], device_id={"tp": peer}, device_id_type=MESH)

    tm_copies = [tmcopy(r) for r in range(1, n)]
    s0.start()
    for c in tm_copies:
        c.start()
    s1.start()
    for c in tm_copies:
        c.wait()

    def block_of(p):
        q = lax.rem(p, 2)
        h = p // 2
        own_core = core + q * sgn
        step = jnp.where(h == 0, 0, jnp.where(h == 1, -sgn, jnp.where(h == 2, sgn, 2)))
        flip = jnp.where(h == 3, 1, 1 - 2 * q)
        return dev(chip + step * flip, own_core)

    def z_copy(nn, buf):
        p, t = nn // tiles, lax.rem(nn, tiles)
        slot = lax.rem(nn, 2)
        return pltpu.make_async_copy(buf, z_hbm.at[block_of(p), pl.ds(pl.multiple_of(t * vt, 16), vt)], z_sem.at[slot])

    def x_out(p):
        b = block_of(p)
        return pltpu.make_async_copy(x_all.at[b], x_hbm.at[b], xo_sem.at[p])

    def reset():
        m_run[...] = jnp.full_like(m_run, NEG)
        m_old[...] = jnp.full_like(m_old, NEG)
        s_run[...] = jnp.zeros_like(s_run)
        t_run[...] = jnp.zeros_like(t_run)

    sub = lax.broadcasted_iota(jnp.int32, (8, tok), 0)

    def sums_begin(nn):
        p, t = nn // tiles, lax.rem(nn, tiles)
        want = tm_all[block_of(p)][0:1] - (me * vocab + t * vt) - sub
        m = m_run[...]
        return want, m, s_run[...] * jnp.exp(m_old[...] - m), t_run[...]

    def sums_rows(acc, buf, start, count):
        want, m, s, tgt = acc
        for lo, size in row_chunks(count, STAT_ROWS):
            z = buf[start + lo:start + lo + size, :].reshape(size // 8, 8, tok)
            s = s + jnp.sum(jnp.exp(z - m[None]), axis=0)
            rows = lax.broadcasted_iota(jnp.int32, z.shape, 0) * 8 + (start + lo)
            tgt = tgt + jnp.sum(jnp.where(want[None] == rows, z, 0.0), axis=0)
        return want, m, s, tgt

    def sums_end(acc):
        _, m_old[...], s_run[...], t_run[...] = acc

    def sums(nn, buf):
        sums_end(sums_rows(sums_begin(nn), buf, 0, vt))

    def st_copy(r, blk):
        peer = lax.rem(me + r, n)
        return pltpu.make_async_remote_copy(src_ref=st_own.at[blk], dst_ref=st_all.at[me, blk], send_sem=st_send.at[r - 1],
                                            recv_sem=st_recv.at[r - 1], device_id={"tp": peer}, device_id_type=MESH)

    def finish(p):
        b = block_of(p)
        m, s = m_run[...], s_run[...]
        m_all = jnp.max(m, axis=0, keepdims=True)
        s_sum = jnp.sum(s * jnp.exp(m - m_all), axis=0, keepdims=True)
        both = jnp.concatenate([m_all + jnp.log(s_sum), jnp.sum(t_run[...], axis=0, keepdims=True)], axis=0)
        st_own[b] = both
        st_all[me, b] = both

    def send_stats(p):
        b = block_of(p)
        for r in range(1, n):
            st_copy(r, b).start()

    reset()

    def step(nn, cur, prev):
        p, t = nn // tiles, lax.rem(nn, tiles)

        @pl.when(t == 0)
        def _():
            @pl.when(p == 1)
            def _():
                s0.wait_recv()

            @pl.when(p == 2)
            def _():
                s1.wait()
                s3.start()
                s2.start()

            @pl.when(p == 3)
            def _():
                s3.wait_recv()
                s4.start()

            @pl.when(p == 4)
            def _():
                s2.wait()
                s5.start()

            @pl.when(p == 5)
            def _():
                s5.wait_recv()

            @pl.when(p == 6)
            def _():
                s4.wait_recv()
                s6.start()

            @pl.when(p == 7)
            def _():
                s6.wait_recv()

            b = block_of(p)
            x_out(p).start()
            x_t[...] = x_all[b].T

        for tt in range(tiles):
            @pl.when(nn == tt)
            def _():
                e_copies[tt].wait()

        @pl.when(nn >= 2)
        def _():
            z_copy(nn - 2, cur).wait()

        top = jnp.full((8, tok), NEG, jnp.float32)
        acc = sums_begin(jnp.maximum(nn - 1, 0))
        for lo, size in row_chunks(vt, DOT_ROWS):
            z = jnp.dot(e_v[pl.ds(pl.multiple_of(t * vt + lo, 16), size), :], x_t[...], preferred_element_type=jnp.float32)
            cur[lo:lo + size, :] = z
            top = jnp.maximum(top, jnp.max(z.reshape(size // 8, 8, tok), axis=0))
            acc = sums_rows(acc, prev, lo, size)
        sums_end(acc)
        z_copy(nn, cur).start()

        @pl.when(t == 0)
        def _():
            @pl.when(nn > 0)
            def _():
                finish(p - 1)
            reset()

        m_run[...] = jnp.maximum(m_run[...], top)

        @pl.when((t == 1) & (p > 0))
        def _():
            send_stats(p - 1)

    def body(i, carry):
        step(2 * i, z_a, z_b)
        step(2 * i + 1, z_b, z_a)
        return carry

    total = n * tiles
    lax.fori_loop(0, total // 2, body, 0)
    sums(total - 1, z_b)
    finish(n - 1)
    z_copy(total - 2, z_a).wait()
    send_stats(n - 1)
    z_copy(total - 1, z_b).wait()
    s0.wait_send()
    s3.wait_send()
    s4.wait_send()
    s5.wait_send()
    s6.wait_send()
    for p in range(n):
        x_out(p).wait()

    for r in range(1, n):
        src = lax.rem(me + n - r, n)
        pltpu.make_async_remote_copy(src_ref=st_own, dst_ref=st_all.at[src], send_sem=st_send.at[r - 1],
                                     recv_sem=st_recv.at[r - 1], device_id={"tp": src}, device_id_type=MESH).wait()

    parts = [st_all[d] for d in range(n)]
    lses = [q[:, 0, :] for q in parts]
    top = functools.reduce(jnp.maximum, lses)
    lse = top + jnp.log(sum(jnp.exp(q - top) for q in lses))
    tgt_logit = sum(q[:, 1, :] for q in parts)
    tm_full = tm_all[...]
    mask = tm_full[:, 1, :].astype(jnp.float32)
    count = jnp.sum(mask)
    loss = (lse - tgt_logit) * mask
    half = tok // 2
    for d in range(n):
        for h in range(2):
            part = slice(h * half, (h + 1) * half)
            lse_o[2 * d + h] = lse[d:d + 1, part]
            scale_o[2 * d + h] = mask[d:d + 1, part] / count
            tgt_o[2 * d + h] = tm_full[d, 0:1, part] - me * vocab
    own = lax.broadcasted_iota(jnp.int32, loss.shape, 0) == me
    loss_o[...] = jnp.sum(jnp.where(own, loss, 0.0), axis=0, keepdims=True)
    mean_o[...] = jnp.full(mean_o.shape, jnp.sum(loss) / count, jnp.float32)


def forward(n, hidden, tm, ln_params, out_embed):
    tok, dim = hidden.shape
    vocab = out_embed.shape[0]
    tiles = 3
    vt = vocab // tiles
    vmem = pl.BlockSpec(memory_space=pltpu.VMEM)
    hbm = pl.BlockSpec(memory_space=pl.ANY)
    f32, bf16, i32 = jnp.float32, jnp.bfloat16, jnp.int32
    dma = pltpu.SemaphoreType.DMA
    return pl.pallas_call(
        functools.partial(forward_kernel, n, tiles),
        name="forward",
        out_shape=(
            jax.ShapeDtypeStruct((n, vocab, tok), f32),
            jax.ShapeDtypeStruct((n, tok, dim), bf16),
            jax.ShapeDtypeStruct((2 * n, 1, tok // 2), f32),
            jax.ShapeDtypeStruct((2 * n, 1, tok // 2), f32),
            jax.ShapeDtypeStruct((2 * n, 1, tok // 2), i32),
            jax.ShapeDtypeStruct((1, tok), f32),
            jax.ShapeDtypeStruct((1, 128), f32),
        ),
        in_specs=[vmem, vmem, vmem, hbm],
        out_specs=(hbm, hbm, vmem, vmem, vmem, vmem, vmem),
        scratch_shapes=[
            pltpu.VMEM((n, tok, dim), bf16),
            pltpu.VMEM((tok, dim), bf16),
            pltpu.VMEM((n, 2, tok), i32),
            pltpu.VMEM((vocab, dim), bf16),
            pltpu.VMEM((dim, tok), bf16),
            pltpu.VMEM((vt, tok), f32),
            pltpu.VMEM((vt, tok), f32),
            pltpu.VMEM((8, tok), f32),
            pltpu.VMEM((8, tok), f32),
            pltpu.VMEM((8, tok), f32),
            pltpu.VMEM((8, tok), f32),
            pltpu.VMEM((n, 2, tok), f32),
            pltpu.VMEM((n, n, 2, tok), f32),
            dma((tiles,)), dma((2,)), dma((n,)),
            dma((7,)), dma((8,)), dma((n - 1,)), dma((n - 1,)), dma((n - 1,)), dma((n - 1,)),
        ],
        compiler_params=pltpu.CompilerParams(collective_id=0, has_side_effects=True, vmem_limit_bytes=VMEM_LIMIT),
        cost_estimate=pl.CostEstimate(flops=2 * n * tok * dim * vocab, bytes_accessed=4 * n * tok * vocab, transcendentals=n * tok * vocab),
    )(hidden, tm, ln_params, out_embed)


def vocab_parts(vocab):
    size = vocab // 3 // 256 * 256
    return [(0, size), (size, size), (2 * size, vocab - 2 * size)]


def backward_kernel(n, hid, lnp, lse, scale, tgt, z_hbm, e_hbm,
                    dz_hbm, dh_o, dln_o,
                    z_0, z_1, z_2, dz_0, dz_1, dz_2, e_in, e_t, acc, own_part, to_pair, from_pair, to_ring, from_ring, d_ln,
                    z_sem, dz_sem, e_sem, pair_send, pair_recv, ring_send, ring_recv, ln_send, ln_recv):
    me = lax.axis_index("tp")
    chips = n // 2
    chip, core = me // 2, lax.rem(me, 2)
    sgn = 1 - 2 * core
    vocab, half = e_in.shape[0], acc.shape[1] // 2
    z_bufs, dz_bufs = (z_0, z_1, z_2), (dz_0, dz_1, dz_2)
    parts = vocab_parts(vocab)
    rounds = 2 * chips

    def dev(chip_idx, core_idx):
        return lax.rem(chip_idx + 2 * chips, chips) * 2 + core_idx

    partner = dev(chip, 1 - core)
    ahead = dev(chip + sgn, core)

    def block_of(u, own):
        hop = 1 + u // 2
        return dev(chip - sgn * hop, core) if own else dev(chip + sgn * hop, 1 - core)

    def z_copies(u, t):
        lo, size = parts[t]
        cols = pl.ds(pl.multiple_of(lax.rem(u, 2) * half, half), half)
        return [pltpu.make_async_copy(z_hbm.at[block_of(u, own), pl.ds(lo, size), cols], z_bufs[t].at[:, own * half:(own + 1) * half], z_sem.at[t, own])
                for own in range(2)]

    def dz_copies(u, t):
        lo, size = parts[t]
        cols = [pl.ds(pl.multiple_of((block_of(u, own) * 2 + lax.rem(u, 2)) * half, half), half) for own in range(2)]
        return [pltpu.make_async_copy(dz_bufs[t].at[:, own * half:(own + 1) * half], dz_hbm.at[pl.ds(lo, size), cols[own]], dz_sem.at[t, own])
                for own in range(2)]

    def start(copies):
        for c in copies:
            c.start()

    def wait(copies):
        for c in copies:
            c.wait()

    e_copies = [pltpu.make_async_copy(e_hbm.at[pl.ds(lo, size)], e_in.at[pl.ds(lo, size)], e_sem.at[k]) for k, (lo, size) in enumerate(parts)]
    start(e_copies)
    for t in range(len(parts)):
        start(z_copies(0, t))

    barrier = pltpu.get_barrier_semaphore()
    for r in range(1, n):
        pl.semaphore_signal(barrier, inc=1, device_id={"tp": lax.rem(me + r, n)}, device_id_type=MESH)
    for c, (lo, size) in zip(e_copies, parts):
        c.wait()
        e_t[:, lo:lo + size] = e_in[lo:lo + size, :].T
    pl.semaphore_wait(barrier, n - 1)

    def pair_copy(u):
        return pltpu.make_async_remote_copy(src_ref=to_pair.at[lax.rem(u, 2)], dst_ref=from_pair.at[u], send_sem=pair_send.at[u],
                                            recv_sem=pair_recv.at[u], device_id={"tp": partner}, device_id_type=MESH)

    def ring_copy(u):
        return pltpu.make_async_remote_copy(src_ref=to_ring.at[lax.rem(u, 2)], dst_ref=from_ring.at[u], send_sem=ring_send.at[u],
                                            recv_sem=ring_recv.at[u], device_id={"tp": ahead}, device_id_type=MESH)

    def combine(u):
        slot = lax.rem(u, 2)
        pair_copy(u).wait_recv()

        @pl.when(u < 2)
        def _():
            to_ring[slot] = own_part[slot] + from_pair[u]
            ring_copy(u).start()

        @pl.when((u >= 2) & (u < rounds - 2))
        def _():
            ring_copy(u - 2).wait()
            to_ring[slot] = own_part[slot] + from_pair[u] + from_ring[u - 2]
            ring_copy(u).start()

        @pl.when(u >= rounds - 2)
        def _():
            ring_copy(u - 2).wait()
            to_ring[slot] = own_part[slot] + from_pair[u] + from_ring[u - 2]

    def body(u, carry):
        slot = lax.rem(u, 2)
        both = [block_of(u, own) * 2 + slot for own in range(2)]
        l, sc, want = (jnp.concatenate([ref[both[0]], ref[both[1]]], axis=1) for ref in (lse, scale, tgt))
        for t, (first, count) in enumerate(parts):
            z, dz = z_bufs[t], dz_bufs[t]

            @pl.when(u > 0)
            def _():
                wait(dz_copies(u - 1, t))

            wait(z_copies(u, t))
            seek = want - first
            for lo, size in row_chunks(count, DZ_ROWS):
                rows = lax.broadcasted_iota(jnp.int32, (size, 2 * half), 0) + lo
                hot = jnp.where(rows == seek, 1.0, 0.0)
                dz[lo:lo + size, :] = ((jnp.exp(z[lo:lo + size, :] - l) - hot) * sc).astype(jnp.bfloat16)
            part = jnp.dot(e_t[:, first:first + count], dz[...], preferred_element_type=jnp.float32)
            acc[...] = part if t == 0 else acc[...] + part
            start(dz_copies(u, t))

            @pl.when(u < rounds - 1)
            def _():
                start(z_copies(u + 1, t))

        @pl.when(u > 0)
        def _():
            combine(u - 1)

        @pl.when(u >= 2)
        def _():
            pair_copy(u - 2).wait_send()
        to_pair[slot] = acc[:, :half]
        own_part[slot] = acc[:, half:]
        pair_copy(u).start()
        return carry

    lax.fori_loop(0, rounds, body, 0)
    combine(rounds - 1)
    for u in (rounds - 2, rounds - 1):
        pair_copy(u).wait_send()
    for t in range(len(parts)):
        wait(dz_copies(rounds - 1, t))

    d_x = jnp.concatenate([to_ring[0].T, to_ring[1].T], axis=0)
    rows = hid[...].astype(jnp.float32)
    centered = rows - jnp.mean(rows, axis=-1, keepdims=True)
    rstd = lax.rsqrt(jnp.mean(centered * centered, axis=-1, keepdims=True) + LN_EPS)
    normed = centered * rstd
    d_ln[me] = jnp.concatenate([jnp.sum(d_x * normed, axis=0, keepdims=True), jnp.sum(d_x, axis=0, keepdims=True)], axis=0)

    def ln_copy(r, slot, peer):
        return pltpu.make_async_remote_copy(src_ref=d_ln.at[slot], dst_ref=d_ln.at[slot], send_sem=ln_send.at[r - 1],
                                            recv_sem=ln_recv.at[r - 1], device_id={"tp": peer}, device_id_type=MESH)

    d_normed = d_x * lnp[0:1, :]
    proj = jnp.mean(d_normed * normed, axis=-1, keepdims=True)
    dh_o[...] = (rstd * (d_normed - jnp.mean(d_normed, axis=-1, keepdims=True) - normed * proj)).astype(jnp.bfloat16)
    for r in range(1, n):
        ln_copy(r, me, lax.rem(me + r, n)).start()
    for r in range(1, n):
        src = lax.rem(me + n - r, n)
        ln_copy(r, src, src).wait()
    grad = d_ln[0]
    for d in range(1, n):
        grad = grad + d_ln[d]
    dln_o[...] = grad


def backward(n, hidden, ln_params, lse, scale, tgt, z, out_embed):
    tok, dim = hidden.shape
    vocab = out_embed.shape[0]
    half = tok // 2
    f32, bf16 = jnp.float32, jnp.bfloat16
    vmem = pl.BlockSpec(memory_space=pltpu.VMEM)
    hbm = pl.BlockSpec(memory_space=pl.ANY)
    dma = pltpu.SemaphoreType.DMA
    return pl.pallas_call(
        functools.partial(backward_kernel, n),
        name="backward",
        out_shape=(
            jax.ShapeDtypeStruct((vocab, n * tok), bf16),
            jax.ShapeDtypeStruct((tok, dim), bf16),
            jax.ShapeDtypeStruct((2, dim), f32),
        ),
        in_specs=[vmem] * 5 + [hbm, hbm],
        out_specs=(hbm, vmem, vmem),
        scratch_shapes=[pltpu.VMEM((size, tok), f32) for _, size in vocab_parts(vocab)] + [pltpu.VMEM((size, tok), bf16) for _, size in vocab_parts(vocab)] + [
            pltpu.VMEM((vocab, dim), bf16),
            pltpu.VMEM((dim, vocab), bf16),
            pltpu.VMEM((dim, tok), f32),
            pltpu.VMEM((2, dim, half), f32),
            pltpu.VMEM((2, dim, half), f32),
            pltpu.VMEM((n, dim, half), f32),
            pltpu.VMEM((2, dim, half), f32),
            pltpu.VMEM((n - 2, dim, half), f32),
            pltpu.VMEM((n, 2, dim), f32),
            dma((3, 2)), dma((3, 2)), dma((3,)),
            dma((n,)), dma((n,)), dma((n - 2,)), dma((n - 2,)), dma((n - 1,)), dma((n - 1,)),
        ],
        compiler_params=pltpu.CompilerParams(collective_id=1, has_side_effects=True, vmem_limit_bytes=66_000_000),
        cost_estimate=pl.CostEstimate(flops=2 * n * tok * dim * vocab, bytes_accessed=6 * n * tok * vocab, transcendentals=n * tok * vocab),
    )(hidden, ln_params, lse, scale, tgt, z, out_embed)


def update_kernel(dz, x, e, m, v, e_o, m_o, v_o, grad):
    grad[...] = jnp.dot(dz[...], x[...], preferred_element_type=jnp.float32)
    for lo, size in row_chunks(grad.shape[0], ADAM_ROWS):
        part = slice(lo, lo + size)
        new_e, m_o[part, :], v_o[part, :] = adam_step(e[part, :].astype(jnp.float32), grad[part, :], m[part, :], v[part, :], WEIGHT_DECAY)
        e_o[part, :] = new_e.astype(jnp.bfloat16)


def update(dz, x, out_embed, mom1, mom2):
    vocab, dim = out_embed.shape
    toks = x.shape[0]
    vt = 640
    f32, bf16 = jnp.float32, jnp.bfloat16
    tile = pl.BlockSpec((vt, dim), lambda i: (i, 0))
    return pl.pallas_call(
        update_kernel,
        name="update",
        grid=(pl.cdiv(vocab, vt),),
        in_specs=[pl.BlockSpec((vt, toks), lambda i: (i, 0)), pl.BlockSpec((toks, dim), lambda i: (0, 0)), tile, tile, tile],
        out_specs=(tile, tile, tile),
        out_shape=(jax.ShapeDtypeStruct((vocab, dim), bf16), jax.ShapeDtypeStruct((vocab, dim), f32), jax.ShapeDtypeStruct((vocab, dim), f32)),
        scratch_shapes=[pltpu.VMEM((vt, dim), f32)],
        compiler_params=pltpu.CompilerParams(vmem_limit_bytes=VMEM_LIMIT, dimension_semantics=("arbitrary",)),
        cost_estimate=pl.CostEstimate(flops=2 * toks * dim * vocab, bytes_accessed=2 * toks * vocab + 20 * vocab * dim, transcendentals=2 * vocab * dim),
    )(dz, x, out_embed, mom1, mom2)


def solution(mesh):
    n = mesh.shape["tp"]
    row_spec = P(("dp", "tp"), None)
    tok_spec = P(("dp", "tp"))
    vocab_spec = P("tp", None)
    repl_spec = P()
    part_spec = P("dp", None)

    def device_step(hidden, targets, loss_mask, ln_params, out_embed, ln_mom1, ln_mom2, embed_mom1, embed_mom2):
        tok, dim = hidden.shape
        tm = jnp.stack([targets, loss_mask])
        z, x_full, lse, scale, tgt, loss, mean = forward(n, hidden, tm, ln_params, out_embed)
        dz, d_hidden, d_ln = backward(n, hidden, ln_params, lse, scale, tgt, z, out_embed)
        ln_new, ln_mom1_new, ln_mom2_new = adam_step(ln_params, d_ln, ln_mom1, ln_mom2, 0.0)
        embed_new, embed_mom1_new, embed_mom2_new = update(dz, x_full.reshape(n * tok, dim), out_embed, embed_mom1, embed_mom2)
        return (loss.reshape(tok), mean[0, :1], d_hidden, ln_new, ln_mom1_new, ln_mom2_new, embed_new, embed_mom1_new, embed_mom2_new)

    return jax.shard_map(device_step, mesh=mesh, in_specs=(row_spec, tok_spec, tok_spec, repl_spec, vocab_spec, repl_spec, repl_spec, vocab_spec, vocab_spec), out_specs=(tok_spec, P("dp"), row_spec, part_spec, part_spec, part_spec, row_spec, row_spec, row_spec), check_vma=False)
```

```python
import functools

import jax
import jax.numpy as jnp
from jax import lax
from jax.experimental import pallas as pl
from jax.experimental.pallas import tpu as pltpu
from jax.sharding import PartitionSpec as P

LN_EPS = 1e-5
BETA_ONE = 0.9
BETA_TWO = 0.95
ADAM_EPS = 1e-8
LEARN_RATE = 1e-3
WEIGHT_DECAY = 0.1
ADAM_STEP = 10

MESH = pl.DeviceIdType.MESH
VMEM_LIMIT = 64_000_000
NEG = -3.0e38
STAT_ROWS = 64
ADAM_ROWS = 16
DZ_ROWS = 64
DOT_ROWS = 1056


def layer_norm(hidden, ln_params):
    rows_f32 = hidden.astype(jnp.float32)
    row_mean = jnp.mean(rows_f32, axis=-1, keepdims=True)
    centered = rows_f32 - row_mean
    row_var = jnp.mean(centered * centered, axis=-1, keepdims=True)
    normed = centered * lax.rsqrt(row_var + LN_EPS)
    return normed * ln_params[0:1] + ln_params[1:2]


def adam_step(param_val, grad_val, m_old, v_old, decay_rate):
    m_new = BETA_ONE * m_old + (1.0 - BETA_ONE) * grad_val
    v_new = BETA_TWO * v_old + (1.0 - BETA_TWO) * grad_val * grad_val
    m_step = m_new * (LEARN_RATE / (1.0 - BETA_ONE ** ADAM_STEP))
    v_hat = v_new * (1.0 / (1.0 - BETA_TWO ** ADAM_STEP))
    new_param = (1.0 - LEARN_RATE * decay_rate) * param_val - m_step / (jnp.sqrt(v_hat) + ADAM_EPS)
    return new_param, m_new, v_new


def row_chunks(rows, size):
    return [(lo, min(size, rows - lo)) for lo in range(0, rows, size)]


def forward_kernel(n, tiles, hid, tm, lnp, e_hbm,
                   z_hbm, x_hbm, lse_o, scale_o, tgt_o, loss_o, mean_o,
                   x_all, x_send, tm_all, e_v, x_t, z_a, z_b, m_run, m_old, s_run, t_run, st_own, st_all,
                   e_sem, z_sem, xo_sem, sx_send, sx_recv, tm_send, tm_recv, st_send, st_recv):
    me = lax.axis_index("tp")
    chips = n // 2
    chip, core = me // 2, lax.rem(me, 2)
    sgn = 1 - 2 * core
    tok = hid.shape[0]
    vocab = e_hbm.shape[0]
    vt = vocab // tiles

    def dev(chip_idx, core_idx):
        return lax.rem(chip_idx + 2 * chips, chips) * 2 + core_idx

    e_copies = [pltpu.make_async_copy(e_hbm.at[pl.ds(t * vt, vt)], e_v.at[pl.ds(t * vt, vt)], e_sem.at[t]) for t in range(tiles)]
    for c in e_copies:
        c.start()

    barrier = pltpu.get_barrier_semaphore()
    for r in range(1, n):
        pl.semaphore_signal(barrier, inc=1, device_id={"tp": lax.rem(me + r, n)}, device_id_type=MESH)

    x_send[...] = layer_norm(hid[...], lnp[...]).astype(jnp.bfloat16)
    x_all[me] = x_send[...]
    tm_all[me] = tm[...]
    pl.semaphore_wait(barrier, n - 1)

    def xcopy(idx, src, slot, dst, recv):
        return pltpu.make_async_remote_copy(src_ref=src, dst_ref=x_all.at[slot], send_sem=sx_send.at[idx],
                                            recv_sem=sx_recv.at[recv], device_id={"tp": dst}, device_id_type=MESH)

    partner = dev(chip, 1 - core)
    ahead = dev(chip + sgn, core)
    behind = dev(chip - sgn, core)
    a1 = dev(chip - sgn, core)
    a2 = dev(chip + sgn, core)
    far = dev(chip + 2, core)
    s0 = xcopy(0, x_send, me, partner, 1)
    s1 = xcopy(1, x_send, me, ahead, 2)
    s2 = xcopy(2, x_send, me, behind, 4)
    s3 = xcopy(3, x_all.at[a1], a1, partner, 3)
    s4 = xcopy(4, x_all.at[a1], a1, ahead, 6)
    s5 = xcopy(5, x_all.at[a2], a2, partner, 5)
    s6 = xcopy(6, x_all.at[far], far, partner, 7)

    def tmcopy(r):
        peer = lax.rem(me + r, n)
        return pltpu.make_async_remote_copy(src_ref=tm, dst_ref=tm_all.at[me], send_sem=tm_send.at[r - 1],
                                            recv_sem=tm_recv.at[r - 1], device_id={"tp": peer}, device_id_type=MESH)

    tm_copies = [tmcopy(r) for r in range(1, n)]
    s0.start()
    for c in tm_copies:
        c.start()
    s1.start()
    for c in tm_copies:
        c.wait()

    def block_of(p):
        q = lax.rem(p, 2)
        h = p // 2
        own_core = core + q * sgn
        step = jnp.where(h == 0, 0, jnp.where(h == 1, -sgn, jnp.where(h == 2, sgn, 2)))
        flip = jnp.where(h == 3, 1, 1 - 2 * q)
        return dev(chip + step * flip, own_core)

    def z_copy(nn, buf):
        p, t = nn // tiles, lax.rem(nn, tiles)
        slot = lax.rem(nn, 2)
        return pltpu.make_async_copy(buf, z_hbm.at[pl.ds(2 * block_of(p), 2), pl.ds(pl.multiple_of(t * vt, 16), vt)], z_sem.at[slot])

    def x_out(p):
        b = block_of(p)
        return pltpu.make_async_copy(x_all.at[b], x_hbm.at[b], xo_sem.at[p])

    def reset():
        m_run[...] = jnp.full_like(m_run, NEG)
        m_old[...] = jnp.full_like(m_old, NEG)
        s_run[...] = jnp.zeros_like(s_run)
        t_run[...] = jnp.zeros_like(t_run)

    sub = lax.broadcasted_iota(jnp.int32, (8, tok), 0)

    def sums_begin(nn):
        p, t = nn // tiles, lax.rem(nn, tiles)
        want = tm_all[block_of(p)][0:1] - (me * vocab + t * vt) - sub
        m = m_run[...]
        return want, m, s_run[...] * jnp.exp(m_old[...] - m), t_run[...]

    def sums_rows(acc, buf, start, count):
        want, m, s, tgt = acc
        for lo, size in row_chunks(count, STAT_ROWS):
            part = slice(start + lo, start + lo + size)
            z = jnp.concatenate([buf[0, part, :], buf[1, part, :]], axis=1).reshape(size // 8, 8, tok)
            s = s + jnp.sum(jnp.exp(z - m[None]), axis=0)
            rows = lax.broadcasted_iota(jnp.int32, z.shape, 0) * 8 + (start + lo)
            tgt = tgt + jnp.sum(jnp.where(want[None] == rows, z, 0.0), axis=0)
        return want, m, s, tgt

    def sums_end(acc):
        _, m_old[...], s_run[...], t_run[...] = acc

    def sums(nn, buf):
        sums_end(sums_rows(sums_begin(nn), buf, 0, vt))

    def st_copy(r, blk):
        peer = lax.rem(me + r, n)
        return pltpu.make_async_remote_copy(src_ref=st_own.at[blk], dst_ref=st_all.at[me, blk], send_sem=st_send.at[r - 1],
                                            recv_sem=st_recv.at[r - 1], device_id={"tp": peer}, device_id_type=MESH)

    def finish(p):
        b = block_of(p)
        m, s = m_run[...], s_run[...]
        m_all = jnp.max(m, axis=0, keepdims=True)
        s_sum = jnp.sum(s * jnp.exp(m - m_all), axis=0, keepdims=True)
        both = jnp.concatenate([m_all + jnp.log(s_sum), jnp.sum(t_run[...], axis=0, keepdims=True)], axis=0)
        st_own[b] = both
        st_all[me, b] = both

    def send_stats(p):
        b = block_of(p)
        for r in range(1, n):
            st_copy(r, b).start()

    reset()

    def step(nn, cur, prev):
        p, t = nn // tiles, lax.rem(nn, tiles)

        @pl.when(t == 0)
        def _():
            @pl.when(p == 1)
            def _():
                s0.wait_recv()

            @pl.when(p == 2)
            def _():
                s1.wait()
                s3.start()
                s2.start()

            @pl.when(p == 3)
            def _():
                s3.wait_recv()
                s4.start()

            @pl.when(p == 4)
            def _():
                s2.wait()
                s5.start()

            @pl.when(p == 5)
            def _():
                s5.wait_recv()

            @pl.when(p == 6)
            def _():
                s4.wait_recv()
                s6.start()

            @pl.when(p == 7)
            def _():
                s6.wait_recv()

            b = block_of(p)
            x_out(p).start()
            x_t[...] = x_all[b].T

        for tt in range(tiles):
            @pl.when(nn == tt)
            def _():
                e_copies[tt].wait()

        @pl.when(nn >= 2)
        def _():
            z_copy(nn - 2, cur).wait()

        top = jnp.full((8, tok), NEG, jnp.float32)
        acc = sums_begin(jnp.maximum(nn - 1, 0))
        for lo, size in row_chunks(vt, DOT_ROWS):
            z = jnp.dot(e_v[pl.ds(pl.multiple_of(t * vt + lo, 16), size), :], x_t[...], preferred_element_type=jnp.float32)
            cur[0, lo:lo + size, :] = z[:, :tok // 2]
            cur[1, lo:lo + size, :] = z[:, tok // 2:]
            top = jnp.maximum(top, jnp.max(z.reshape(size // 8, 8, tok), axis=0))
            acc = sums_rows(acc, prev, lo, size)
        sums_end(acc)
        z_copy(nn, cur).start()

        @pl.when(t == 0)
        def _():
            @pl.when(nn > 0)
            def _():
                finish(p - 1)
            reset()

        m_run[...] = jnp.maximum(m_run[...], top)

        @pl.when((t == 1) & (p > 0))
        def _():
            send_stats(p - 1)

    def body(i, carry):
        step(2 * i, z_a, z_b)
        step(2 * i + 1, z_b, z_a)
        return carry

    total = n * tiles
    lax.fori_loop(0, total // 2, body, 0)
    sums(total - 1, z_b)
    finish(n - 1)
    z_copy(total - 2, z_a).wait()
    send_stats(n - 1)
    z_copy(total - 1, z_b).wait()
    s0.wait_send()
    s3.wait_send()
    s4.wait_send()
    s5.wait_send()
    s6.wait_send()
    for p in range(n):
        x_out(p).wait()

    for r in range(1, n):
        src = lax.rem(me + n - r, n)
        pltpu.make_async_remote_copy(src_ref=st_own, dst_ref=st_all.at[src], send_sem=st_send.at[r - 1],
                                     recv_sem=st_recv.at[r - 1], device_id={"tp": src}, device_id_type=MESH).wait()

    parts = [st_all[d] for d in range(n)]
    lses = [q[:, 0, :] for q in parts]
    top = functools.reduce(jnp.maximum, lses)
    lse = top + jnp.log(sum(jnp.exp(q - top) for q in lses))
    tgt_logit = sum(q[:, 1, :] for q in parts)
    tm_full = tm_all[...]
    mask = tm_full[:, 1, :].astype(jnp.float32)
    count = jnp.sum(mask)
    loss = (lse - tgt_logit) * mask
    half = tok // 2
    for d in range(n):
        for h in range(2):
            part = slice(h * half, (h + 1) * half)
            lse_o[2 * d + h] = lse[d:d + 1, part]
            scale_o[2 * d + h] = mask[d:d + 1, part] / count
            tgt_o[2 * d + h] = tm_full[d, 0:1, part] - me * vocab
    own = lax.broadcasted_iota(jnp.int32, loss.shape, 0) == me
    loss_o[...] = jnp.sum(jnp.where(own, loss, 0.0), axis=0, keepdims=True)
    mean_o[...] = jnp.full(mean_o.shape, jnp.sum(loss) / count, jnp.float32)


def forward(n, hidden, tm, ln_params, out_embed):
    tok, dim = hidden.shape
    vocab = out_embed.shape[0]
    tiles = 3
    vt = vocab // tiles
    vmem = pl.BlockSpec(memory_space=pltpu.VMEM)
    hbm = pl.BlockSpec(memory_space=pl.ANY)
    f32, bf16, i32 = jnp.float32, jnp.bfloat16, jnp.int32
    dma = pltpu.SemaphoreType.DMA
    return pl.pallas_call(
        functools.partial(forward_kernel, n, tiles),
        name="forward",
        out_shape=(
            jax.ShapeDtypeStruct((2 * n, vocab, tok // 2), f32),
            jax.ShapeDtypeStruct((n, tok, dim), bf16),
            jax.ShapeDtypeStruct((2 * n, 1, tok // 2), f32),
            jax.ShapeDtypeStruct((2 * n, 1, tok // 2), f32),
            jax.ShapeDtypeStruct((2 * n, 1, tok // 2), i32),
            jax.ShapeDtypeStruct((1, tok), f32),
            jax.ShapeDtypeStruct((1, 128), f32),
        ),
        in_specs=[vmem, vmem, vmem, hbm],
        out_specs=(hbm, hbm, vmem, vmem, vmem, vmem, vmem),
        scratch_shapes=[
            pltpu.VMEM((n, tok, dim), bf16),
            pltpu.VMEM((tok, dim), bf16),
            pltpu.VMEM((n, 2, tok), i32),
            pltpu.VMEM((vocab, dim), bf16),
            pltpu.VMEM((dim, tok), bf16),
            pltpu.VMEM((2, vt, tok // 2), f32),
            pltpu.VMEM((2, vt, tok // 2), f32),
            pltpu.VMEM((8, tok), f32),
            pltpu.VMEM((8, tok), f32),
            pltpu.VMEM((8, tok), f32),
            pltpu.VMEM((8, tok), f32),
            pltpu.VMEM((n, 2, tok), f32),
            pltpu.VMEM((n, n, 2, tok), f32),
            dma((tiles,)), dma((2,)), dma((n,)),
            dma((7,)), dma((8,)), dma((n - 1,)), dma((n - 1,)), dma((n - 1,)), dma((n - 1,)),
        ],
        compiler_params=pltpu.CompilerParams(collective_id=0, has_side_effects=True, vmem_limit_bytes=VMEM_LIMIT),
        cost_estimate=pl.CostEstimate(flops=2 * n * tok * dim * vocab, bytes_accessed=4 * n * tok * vocab, transcendentals=n * tok * vocab),
    )(hidden, tm, ln_params, out_embed)


def vocab_parts(vocab):
    size = vocab // 3 // 256 * 256
    return [(0, size), (size, size), (2 * size, vocab - 2 * size)]


def backward_kernel(n, hid, lnp, lse, scale, tgt, z_hbm, e_hbm,
                    dz_hbm, dh_o, dln_o,
                    z_0, z_1, z_2, dz_0, dz_1, dz_2, e_in, e_t, acc, own_part, to_pair, from_pair, to_ring, from_ring, d_ln,
                    z_sem, dz_sem, e_sem, pair_send, pair_recv, ring_send, ring_recv, ln_send, ln_recv):
    me = lax.axis_index("tp")
    chips = n // 2
    chip, core = me // 2, lax.rem(me, 2)
    sgn = 1 - 2 * core
    vocab, half = e_in.shape[0], acc.shape[1] // 2
    z_bufs, dz_bufs = (z_0, z_1, z_2), (dz_0, dz_1, dz_2)
    parts = vocab_parts(vocab)
    rounds = 2 * chips

    def dev(chip_idx, core_idx):
        return lax.rem(chip_idx + 2 * chips, chips) * 2 + core_idx

    partner = dev(chip, 1 - core)
    ahead = dev(chip + sgn, core)

    def block_of(u, own):
        hop = 1 + u // 2
        return dev(chip - sgn * hop, core) if own else dev(chip + sgn * hop, 1 - core)

    def z_copies(u, t):
        lo, size = parts[t]
        return [pltpu.make_async_copy(z_hbm.at[block_of(u, own) * 2 + lax.rem(u, 2), pl.ds(lo, size)], z_bufs[t].at[own], z_sem.at[t, own])
                for own in range(2)]

    def dz_copies(u, t):
        lo, size = parts[t]
        return [pltpu.make_async_copy(dz_bufs[t].at[own], dz_hbm.at[block_of(u, own) * 2 + lax.rem(u, 2), pl.ds(lo, size)], dz_sem.at[t, own])
                for own in range(2)]

    def start(copies):
        for c in copies:
            c.start()

    def wait(copies):
        for c in copies:
            c.wait()

    e_copies = [pltpu.make_async_copy(e_hbm.at[pl.ds(lo, size)], e_in.at[pl.ds(lo, size)], e_sem.at[k]) for k, (lo, size) in enumerate(parts)]
    start(e_copies)
    for t in range(len(parts)):
        start(z_copies(0, t))

    barrier = pltpu.get_barrier_semaphore()
    for r in range(1, n):
        pl.semaphore_signal(barrier, inc=1, device_id={"tp": lax.rem(me + r, n)}, device_id_type=MESH)
    for c, (lo, size) in zip(e_copies, parts):
        c.wait()
        e_t[:, lo:lo + size] = e_in[lo:lo + size, :].T
    pl.semaphore_wait(barrier, n - 1)

    def pair_copy(u):
        return pltpu.make_async_remote_copy(src_ref=to_pair.at[lax.rem(u, 2)], dst_ref=from_pair.at[u], send_sem=pair_send.at[u],
                                            recv_sem=pair_recv.at[u], device_id={"tp": partner}, device_id_type=MESH)

    def ring_copy(u):
        return pltpu.make_async_remote_copy(src_ref=to_ring.at[lax.rem(u, 2)], dst_ref=from_ring.at[u], send_sem=ring_send.at[u],
                                            recv_sem=ring_recv.at[u], device_id={"tp": ahead}, device_id_type=MESH)

    def combine(u):
        slot = lax.rem(u, 2)
        pair_copy(u).wait_recv()

        @pl.when(u < 2)
        def _():
            to_ring[slot] = own_part[slot] + from_pair[u]
            ring_copy(u).start()

        @pl.when((u >= 2) & (u < rounds - 2))
        def _():
            ring_copy(u - 2).wait()
            to_ring[slot] = own_part[slot] + from_pair[u] + from_ring[u - 2]
            ring_copy(u).start()

        @pl.when(u >= rounds - 2)
        def _():
            ring_copy(u - 2).wait()
            to_ring[slot] = own_part[slot] + from_pair[u] + from_ring[u - 2]

    def body(u, carry):
        slot = lax.rem(u, 2)
        both = [block_of(u, own) * 2 + slot for own in range(2)]
        stats = [(lse[row], scale[row], tgt[row]) for row in both]
        for t, (first, count) in enumerate(parts):
            z, dz = z_bufs[t], dz_bufs[t]

            @pl.when(u > 0)
            def _():
                wait(dz_copies(u - 1, t))

            wait(z_copies(u, t))
            for lo, size in row_chunks(count, DZ_ROWS):
                rows = lax.broadcasted_iota(jnp.int32, (size, half), 0) + lo
                for own, (l, sc, want) in enumerate(stats):
                    hot = jnp.where(rows == want - first, 1.0, 0.0)
                    dz[own, lo:lo + size, :] = ((jnp.exp(z[own, lo:lo + size, :] - l) - hot) * sc).astype(jnp.bfloat16)
            both_dz = jnp.concatenate([dz[0], dz[1]], axis=1)
            part = jnp.dot(e_t[:, first:first + count], both_dz, preferred_element_type=jnp.float32)
            acc[...] = part if t == 0 else acc[...] + part
            start(dz_copies(u, t))

            @pl.when(u < rounds - 1)
            def _():
                start(z_copies(u + 1, t))

        @pl.when(u > 0)
        def _():
            combine(u - 1)

        @pl.when(u >= 2)
        def _():
            pair_copy(u - 2).wait_send()
        to_pair[slot] = acc[:, :half]
        own_part[slot] = acc[:, half:]
        pair_copy(u).start()
        return carry

    lax.fori_loop(0, rounds, body, 0)
    combine(rounds - 1)
    for u in (rounds - 2, rounds - 1):
        pair_copy(u).wait_send()
    for t in range(len(parts)):
        wait(dz_copies(rounds - 1, t))

    d_x = jnp.concatenate([to_ring[0].T, to_ring[1].T], axis=0)
    rows = hid[...].astype(jnp.float32)
    centered = rows - jnp.mean(rows, axis=-1, keepdims=True)
    rstd = lax.rsqrt(jnp.mean(centered * centered, axis=-1, keepdims=True) + LN_EPS)
    normed = centered * rstd
    d_ln[me] = jnp.concatenate([jnp.sum(d_x * normed, axis=0, keepdims=True), jnp.sum(d_x, axis=0, keepdims=True)], axis=0)

    def ln_copy(r, slot, peer):
        return pltpu.make_async_remote_copy(src_ref=d_ln.at[slot], dst_ref=d_ln.at[slot], send_sem=ln_send.at[r - 1],
                                            recv_sem=ln_recv.at[r - 1], device_id={"tp": peer}, device_id_type=MESH)

    d_normed = d_x * lnp[0:1, :]
    proj = jnp.mean(d_normed * normed, axis=-1, keepdims=True)
    dh_o[...] = (rstd * (d_normed - jnp.mean(d_normed, axis=-1, keepdims=True) - normed * proj)).astype(jnp.bfloat16)
    for r in range(1, n):
        ln_copy(r, me, lax.rem(me + r, n)).start()
    for r in range(1, n):
        src = lax.rem(me + n - r, n)
        ln_copy(r, src, src).wait()
    grad = d_ln[0]
    for d in range(1, n):
        grad = grad + d_ln[d]
    dln_o[...] = grad


def backward(n, hidden, ln_params, lse, scale, tgt, z, out_embed):
    tok, dim = hidden.shape
    vocab = out_embed.shape[0]
    half = tok // 2
    f32, bf16 = jnp.float32, jnp.bfloat16
    vmem = pl.BlockSpec(memory_space=pltpu.VMEM)
    hbm = pl.BlockSpec(memory_space=pl.ANY)
    dma = pltpu.SemaphoreType.DMA
    return pl.pallas_call(
        functools.partial(backward_kernel, n),
        name="backward",
        out_shape=(
            jax.ShapeDtypeStruct((2 * n, vocab, half), bf16),
            jax.ShapeDtypeStruct((tok, dim), bf16),
            jax.ShapeDtypeStruct((2, dim), f32),
        ),
        in_specs=[vmem] * 5 + [hbm, hbm],
        out_specs=(hbm, vmem, vmem),
        scratch_shapes=[pltpu.VMEM((2, size, half), f32) for _, size in vocab_parts(vocab)] + [pltpu.VMEM((2, size, half), bf16) for _, size in vocab_parts(vocab)] + [
            pltpu.VMEM((vocab, dim), bf16),
            pltpu.VMEM((dim, vocab), bf16),
            pltpu.VMEM((dim, tok), f32),
            pltpu.VMEM((2, dim, half), f32),
            pltpu.VMEM((2, dim, half), f32),
            pltpu.VMEM((n, dim, half), f32),
            pltpu.VMEM((2, dim, half), f32),
            pltpu.VMEM((n - 2, dim, half), f32),
            pltpu.VMEM((n, 2, dim), f32),
            dma((3, 2)), dma((3, 2)), dma((3,)),
            dma((n,)), dma((n,)), dma((n - 2,)), dma((n - 2,)), dma((n - 1,)), dma((n - 1,)),
        ],
        compiler_params=pltpu.CompilerParams(collective_id=1, has_side_effects=True, vmem_limit_bytes=66_000_000),
        cost_estimate=pl.CostEstimate(flops=2 * n * tok * dim * vocab, bytes_accessed=6 * n * tok * vocab, transcendentals=n * tok * vocab),
    )(hidden, ln_params, lse, scale, tgt, z, out_embed)


def update_kernel(dz, x, e, m, v, e_o, m_o, v_o, grad):
    all_dz = jnp.concatenate([dz[j] for j in range(dz.shape[0])], axis=1)
    grad[...] = jnp.dot(all_dz, x[...], preferred_element_type=jnp.float32)
    for lo, size in row_chunks(grad.shape[0], ADAM_ROWS):
        part = slice(lo, lo + size)
        new_e, m_o[part, :], v_o[part, :] = adam_step(e[part, :].astype(jnp.float32), grad[part, :], m[part, :], v[part, :], WEIGHT_DECAY)
        e_o[part, :] = new_e.astype(jnp.bfloat16)


def update(dz, x, out_embed, mom1, mom2):
    vocab, dim = out_embed.shape
    toks = x.shape[0]
    vt = 640
    f32, bf16 = jnp.float32, jnp.bfloat16
    tile = pl.BlockSpec((vt, dim), lambda i: (i, 0))
    return pl.pallas_call(
        update_kernel,
        name="update",
        grid=(pl.cdiv(vocab, vt),),
        in_specs=[pl.BlockSpec((dz.shape[0], vt, dz.shape[2]), lambda i: (0, i, 0)), pl.BlockSpec((toks, dim), lambda i: (0, 0)), tile, tile, tile],
        out_specs=(tile, tile, tile),
        out_shape=(jax.ShapeDtypeStruct((vocab, dim), bf16), jax.ShapeDtypeStruct((vocab, dim), f32), jax.ShapeDtypeStruct((vocab, dim), f32)),
        scratch_shapes=[pltpu.VMEM((vt, dim), f32)],
        compiler_params=pltpu.CompilerParams(vmem_limit_bytes=VMEM_LIMIT, dimension_semantics=("arbitrary",)),
        cost_estimate=pl.CostEstimate(flops=2 * toks * dim * vocab, bytes_accessed=2 * toks * vocab + 20 * vocab * dim, transcendentals=2 * vocab * dim),
    )(dz, x, out_embed, mom1, mom2)


def solution(mesh):
    n = mesh.shape["tp"]
    row_spec = P(("dp", "tp"), None)
    tok_spec = P(("dp", "tp"))
    vocab_spec = P("tp", None)
    repl_spec = P()
    part_spec = P("dp", None)

    def device_step(hidden, targets, loss_mask, ln_params, out_embed, ln_mom1, ln_mom2, embed_mom1, embed_mom2):
        tok, dim = hidden.shape
        tm = jnp.stack([targets, loss_mask])
        z, x_full, lse, scale, tgt, loss, mean = forward(n, hidden, tm, ln_params, out_embed)
        dz, d_hidden, d_ln = backward(n, hidden, ln_params, lse, scale, tgt, z, out_embed)
        ln_new, ln_mom1_new, ln_mom2_new = adam_step(ln_params, d_ln, ln_mom1, ln_mom2, 0.0)
        embed_new, embed_mom1_new, embed_mom2_new = update(dz, x_full.reshape(n * tok, dim), out_embed, embed_mom1, embed_mom2)
        return (loss.reshape(tok), mean[0, :1], d_hidden, ln_new, ln_mom1_new, ln_mom2_new, embed_new, embed_mom1_new, embed_mom2_new)

    return jax.shard_map(device_step, mesh=mesh, in_specs=(row_spec, tok_spec, tok_spec, repl_spec, vocab_spec, repl_spec, repl_spec, vocab_spec, vocab_spec), out_specs=(tok_spec, P("dp"), row_spec, part_spec, part_spec, part_spec, row_spec, row_spec, row_spec), check_vma=False)
```

```python
import functools

import jax
import jax.numpy as jnp
from jax import lax
from jax.experimental import pallas as pl
from jax.experimental.pallas import tpu as pltpu
from jax.sharding import PartitionSpec as P

LN_EPS = 1e-5
BETA_ONE = 0.9
BETA_TWO = 0.95
ADAM_EPS = 1e-8
LEARN_RATE = 1e-3
WEIGHT_DECAY = 0.1
ADAM_STEP = 10

MESH = pl.DeviceIdType.MESH
VMEM_LIMIT = 64_000_000
NEG = -3.0e38
STAT_ROWS = 32
ADAM_ROWS = 16
DZ_ROWS = 64
DOT_ROWS = 1056


def layer_norm(hidden, ln_params):
    rows_f32 = hidden.astype(jnp.float32)
    row_mean = jnp.mean(rows_f32, axis=-1, keepdims=True)
    centered = rows_f32 - row_mean
    row_var = jnp.mean(centered * centered, axis=-1, keepdims=True)
    normed = centered * lax.rsqrt(row_var + LN_EPS)
    return normed * ln_params[0:1] + ln_params[1:2]


def adam_step(param_val, grad_val, m_old, v_old, decay_rate):
    m_new = BETA_ONE * m_old + (1.0 - BETA_ONE) * grad_val
    v_new = BETA_TWO * v_old + (1.0 - BETA_TWO) * grad_val * grad_val
    m_step = m_new * (LEARN_RATE / (1.0 - BETA_ONE ** ADAM_STEP))
    v_hat = v_new * (1.0 / (1.0 - BETA_TWO ** ADAM_STEP))
    new_param = (1.0 - LEARN_RATE * decay_rate) * param_val - m_step / (jnp.sqrt(v_hat) + ADAM_EPS)
    return new_param, m_new, v_new


def row_chunks(rows, size):
    return [(lo, min(size, rows - lo)) for lo in range(0, rows, size)]


def forward_kernel(n, tiles, hid, tm, lnp, e_hbm,
                   z_hbm, x_hbm, lse_o, scale_o, tgt_o, loss_o, mean_o,
                   x_all, x_send, tm_all, e_v, x_t, z_a, z_b, m_run, m_old, s_run, t_run, st_own, st_all,
                   e_sem, z_sem, xo_sem, sx_send, sx_recv, tm_send, tm_recv, st_send, st_recv):
    me = lax.axis_index("tp")
    chips = n // 2
    chip, core = me // 2, lax.rem(me, 2)
    sgn = 1 - 2 * core
    tok = hid.shape[0]
    vocab = e_hbm.shape[0]
    vt = vocab // tiles

    def dev(chip_idx, core_idx):
        return lax.rem(chip_idx + 2 * chips, chips) * 2 + core_idx

    e_copies = [pltpu.make_async_copy(e_hbm.at[pl.ds(t * vt, vt)], e_v.at[pl.ds(t * vt, vt)], e_sem.at[t]) for t in range(tiles)]
    for c in e_copies:
        c.start()

    barrier = pltpu.get_barrier_semaphore()
    for r in range(1, n):
        pl.semaphore_signal(barrier, inc=1, device_id={"tp": lax.rem(me + r, n)}, device_id_type=MESH)

    x_send[...] = layer_norm(hid[...], lnp[...]).astype(jnp.bfloat16)
    x_all[me] = x_send[...]
    tm_all[me] = tm[...]
    pl.semaphore_wait(barrier, n - 1)

    def xcopy(idx, src, slot, dst, recv):
        return pltpu.make_async_remote_copy(src_ref=src, dst_ref=x_all.at[slot], send_sem=sx_send.at[idx],
                                            recv_sem=sx_recv.at[recv], device_id={"tp": dst}, device_id_type=MESH)

    partner = dev(chip, 1 - core)
    ahead = dev(chip + sgn, core)
    behind = dev(chip - sgn, core)
    a1 = dev(chip - sgn, core)
    a2 = dev(chip + sgn, core)
    far = dev(chip + 2, core)
    s0 = xcopy(0, x_send, me, partner, 1)
    s1 = xcopy(1, x_send, me, ahead, 2)
    s2 = xcopy(2, x_send, me, behind, 4)
    s3 = xcopy(3, x_all.at[a1], a1, partner, 3)
    s4 = xcopy(4, x_all.at[a1], a1, ahead, 6)
    s5 = xcopy(5, x_all.at[a2], a2, partner, 5)
    s6 = xcopy(6, x_all.at[far], far, partner, 7)

    def tmcopy(r):
        peer = lax.rem(me + r, n)
        return pltpu.make_async_remote_copy(src_ref=tm, dst_ref=tm_all.at[me], send_sem=tm_send.at[r - 1],
                                            recv_sem=tm_recv.at[r - 1], device_id={"tp": peer}, device_id_type=MESH)

    tm_copies = [tmcopy(r) for r in range(1, n)]
    s0.start()
    for c in tm_copies:
        c.start()
    s1.start()

    def block_of(p):
        q = lax.rem(p, 2)
        h = p // 2
        own_core = core + q * sgn
        step = jnp.where(h == 0, 0, jnp.where(h == 1, -sgn, jnp.where(h == 2, sgn, 2)))
        flip = jnp.where(h == 3, 1, 1 - 2 * q)
        return dev(chip + step * flip, own_core)

    def z_copy(nn, buf):
        p, t = nn // tiles, lax.rem(nn, tiles)
        slot = lax.rem(nn, 2)
        return pltpu.make_async_copy(buf, z_hbm.at[pl.ds(2 * block_of(p), 2), pl.ds(pl.multiple_of(t * vt, 16), vt)], z_sem.at[slot])

    def x_out(p):
        b = block_of(p)
        return pltpu.make_async_copy(x_all.at[b], x_hbm.at[b], xo_sem.at[p])

    def reset():
        m_run[...] = jnp.full_like(m_run, NEG)
        m_old[...] = jnp.full_like(m_old, NEG)
        s_run[...] = jnp.zeros_like(s_run)
        t_run[...] = jnp.zeros_like(t_run)

    sub = lax.broadcasted_iota(jnp.int32, (8, tok), 0)

    def sums_begin(nn):
        p, t = nn // tiles, lax.rem(nn, tiles)
        want = tm_all[block_of(p)][0:1] - (me * vocab + t * vt) - sub
        m = m_run[...]
        return want, m, s_run[...] * jnp.exp(m_old[...] - m), t_run[...]

    def sums_rows(acc, buf, start, count):
        want, m, s, tgt = acc
        for lo, size in row_chunks(count, STAT_ROWS):
            part = slice(start + lo, start + lo + size)
            z = jnp.concatenate([buf[0, part, :], buf[1, part, :]], axis=1).reshape(size // 8, 8, tok)
            s = s + jnp.sum(jnp.exp(z - m[None]), axis=0)
            rows = lax.broadcasted_iota(jnp.int32, z.shape, 0) * 8 + (start + lo)
            tgt = tgt + jnp.sum(jnp.where(want[None] == rows, z, 0.0), axis=0)
        return want, m, s, tgt

    def sums_end(acc):
        _, m_old[...], s_run[...], t_run[...] = acc

    def sums(nn, buf):
        sums_end(sums_rows(sums_begin(nn), buf, 0, vt))

    def st_copy(r, blk):
        peer = lax.rem(me + r, n)
        return pltpu.make_async_remote_copy(src_ref=st_own.at[blk], dst_ref=st_all.at[me, blk], send_sem=st_send.at[r - 1],
                                            recv_sem=st_recv.at[r - 1], device_id={"tp": peer}, device_id_type=MESH)

    def finish(p):
        b = block_of(p)
        m, s = m_run[...], s_run[...]
        m_all = jnp.max(m, axis=0, keepdims=True)
        s_sum = jnp.sum(s * jnp.exp(m - m_all), axis=0, keepdims=True)
        both = jnp.concatenate([m_all + jnp.log(s_sum), jnp.sum(t_run[...], axis=0, keepdims=True)], axis=0)
        st_own[b] = both
        st_all[me, b] = both

    def send_stats(p):
        b = block_of(p)
        for r in range(1, n):
            st_copy(r, b).start()

    reset()

    def step(nn, cur, prev):
        p, t = nn // tiles, lax.rem(nn, tiles)

        @pl.when(t == 0)
        def _():
            @pl.when(p == 1)
            def _():
                for c in tm_copies:
                    c.wait()
                s0.wait_recv()

            @pl.when(p == 2)
            def _():
                s1.wait()
                s3.start()
                s2.start()

            @pl.when(p == 3)
            def _():
                s3.wait_recv()
                s4.start()

            @pl.when(p == 4)
            def _():
                s2.wait()
                s5.start()

            @pl.when(p == 5)
            def _():
                s5.wait_recv()

            @pl.when(p == 6)
            def _():
                s4.wait_recv()
                s6.start()

            @pl.when(p == 7)
            def _():
                s6.wait_recv()

            b = block_of(p)
            x_out(p).start()
            x_t[...] = x_all[b].T

        for tt in range(tiles):
            @pl.when(nn == tt)
            def _():
                e_copies[tt].wait()

        @pl.when(nn >= 2)
        def _():
            z_copy(nn - 2, cur).wait()

        top = jnp.full((8, tok), NEG, jnp.float32)
        acc = sums_begin(jnp.maximum(nn - 1, 0))
        for lo, size in row_chunks(vt, DOT_ROWS):
            z = jnp.dot(e_v[pl.ds(pl.multiple_of(t * vt + lo, 16), size), :], x_t[...], preferred_element_type=jnp.float32)
            cur[0, lo:lo + size, :] = z[:, :tok // 2]
            cur[1, lo:lo + size, :] = z[:, tok // 2:]
            top = jnp.maximum(top, jnp.max(z.reshape(size // 8, 8, tok), axis=0))
            acc = sums_rows(acc, prev, lo, size)
        sums_end(acc)
        z_copy(nn, cur).start()

        @pl.when(t == 0)
        def _():
            @pl.when(nn > 0)
            def _():
                finish(p - 1)
            reset()

        m_run[...] = jnp.maximum(m_run[...], top)

        @pl.when((t == 1) & (p > 0))
        def _():
            send_stats(p - 1)

    def body(i, carry):
        step(2 * i, z_a, z_b)
        step(2 * i + 1, z_b, z_a)
        return carry

    total = n * tiles
    lax.fori_loop(0, total // 2, body, 0)
    sums(total - 1, z_b)
    finish(n - 1)
    z_copy(total - 2, z_a).wait()
    send_stats(n - 1)
    z_copy(total - 1, z_b).wait()
    s0.wait_send()
    s3.wait_send()
    s4.wait_send()
    s5.wait_send()
    s6.wait_send()
    for p in range(n):
        x_out(p).wait()

    for r in range(1, n):
        src = lax.rem(me + n - r, n)
        pltpu.make_async_remote_copy(src_ref=st_own, dst_ref=st_all.at[src], send_sem=st_send.at[r - 1],
                                     recv_sem=st_recv.at[r - 1], device_id={"tp": src}, device_id_type=MESH).wait()

    parts = [st_all[d] for d in range(n)]
    lses = [q[:, 0, :] for q in parts]
    top = functools.reduce(jnp.maximum, lses)
    lse = top + jnp.log(sum(jnp.exp(q - top) for q in lses))
    tgt_logit = sum(q[:, 1, :] for q in parts)
    tm_full = tm_all[...]
    mask = tm_full[:, 1, :].astype(jnp.float32)
    count = jnp.sum(mask)
    loss = (lse - tgt_logit) * mask
    half = tok // 2
    for d in range(n):
        for h in range(2):
            part = slice(h * half, (h + 1) * half)
            lse_o[2 * d + h] = lse[d:d + 1, part]
            scale_o[2 * d + h] = mask[d:d + 1, part] / count
            tgt_o[2 * d + h] = tm_full[d, 0:1, part] - me * vocab
    own = lax.broadcasted_iota(jnp.int32, loss.shape, 0) == me
    loss_o[...] = jnp.sum(jnp.where(own, loss, 0.0), axis=0, keepdims=True)
    mean_o[...] = jnp.full(mean_o.shape, jnp.sum(loss) / count, jnp.float32)


def forward(n, hidden, tm, ln_params, out_embed):
    tok, dim = hidden.shape
    vocab = out_embed.shape[0]
    tiles = 3
    vt = vocab // tiles
    vmem = pl.BlockSpec(memory_space=pltpu.VMEM)
    hbm = pl.BlockSpec(memory_space=pl.ANY)
    f32, bf16, i32 = jnp.float32, jnp.bfloat16, jnp.int32
    dma = pltpu.SemaphoreType.DMA
    return pl.pallas_call(
        functools.partial(forward_kernel, n, tiles),
        name="forward",
        out_shape=(
            jax.ShapeDtypeStruct((2 * n, vocab, tok // 2), f32),
            jax.ShapeDtypeStruct((n, tok, dim), bf16),
            jax.ShapeDtypeStruct((2 * n, 1, tok // 2), f32),
            jax.ShapeDtypeStruct((2 * n, 1, tok // 2), f32),
            jax.ShapeDtypeStruct((2 * n, 1, tok // 2), i32),
            jax.ShapeDtypeStruct((1, tok), f32),
            jax.ShapeDtypeStruct((1, 128), f32),
        ),
        in_specs=[vmem, vmem, vmem, hbm],
        out_specs=(hbm, hbm, vmem, vmem, vmem, vmem, vmem),
        scratch_shapes=[
            pltpu.VMEM((n, tok, dim), bf16),
            pltpu.VMEM((tok, dim), bf16),
            pltpu.VMEM((n, 2, tok), i32),
            pltpu.VMEM((vocab, dim), bf16),
            pltpu.VMEM((dim, tok), bf16),
            pltpu.VMEM((2, vt, tok // 2), f32),
            pltpu.VMEM((2, vt, tok // 2), f32),
            pltpu.VMEM((8, tok), f32),
            pltpu.VMEM((8, tok), f32),
            pltpu.VMEM((8, tok), f32),
            pltpu.VMEM((8, tok), f32),
            pltpu.VMEM((n, 2, tok), f32),
            pltpu.VMEM((n, n, 2, tok), f32),
            dma((tiles,)), dma((2,)), dma((n,)),
            dma((7,)), dma((8,)), dma((n - 1,)), dma((n - 1,)), dma((n - 1,)), dma((n - 1,)),
        ],
        compiler_params=pltpu.CompilerParams(collective_id=0, has_side_effects=True, vmem_limit_bytes=VMEM_LIMIT),
        cost_estimate=pl.CostEstimate(flops=2 * n * tok * dim * vocab, bytes_accessed=4 * n * tok * vocab, transcendentals=n * tok * vocab),
    )(hidden, tm, ln_params, out_embed)


def vocab_parts(vocab):
    size = vocab // 3 // 256 * 256
    return [(0, size), (size, size), (2 * size, vocab - 2 * size)]


def backward_kernel(n, hid, lnp, lse, scale, tgt, z_hbm, e_hbm,
                    dz_hbm, dh_o, dln_o,
                    z_0, z_1, z_2, dz_0, dz_1, dz_2, e_in, e_t, acc, own_part, to_pair, from_pair, to_ring, from_ring, d_ln,
                    z_sem, dz_sem, e_sem, pair_send, pair_recv, ring_send, ring_recv, ln_send, ln_recv):
    me = lax.axis_index("tp")
    chips = n // 2
    chip, core = me // 2, lax.rem(me, 2)
    sgn = 1 - 2 * core
    vocab, half = e_in.shape[0], acc.shape[1] // 2
    z_bufs, dz_bufs = (z_0, z_1, z_2), (dz_0, dz_1, dz_2)
    parts = vocab_parts(vocab)
    rounds = 2 * chips

    def dev(chip_idx, core_idx):
        return lax.rem(chip_idx + 2 * chips, chips) * 2 + core_idx

    partner = dev(chip, 1 - core)
    ahead = dev(chip + sgn, core)

    def block_of(u, own):
        hop = 1 + u // 2
        return dev(chip - sgn * hop, core) if own else dev(chip + sgn * hop, 1 - core)

    def z_copies(u, t):
        lo, size = parts[t]
        return [pltpu.make_async_copy(z_hbm.at[block_of(u, own) * 2 + lax.rem(u, 2), pl.ds(lo, size)], z_bufs[t].at[own], z_sem.at[t, own])
                for own in range(2)]

    def dz_copies(u, t):
        lo, size = parts[t]
        return [pltpu.make_async_copy(dz_bufs[t].at[own], dz_hbm.at[block_of(u, own) * 2 + lax.rem(u, 2), pl.ds(lo, size)], dz_sem.at[t, own])
                for own in range(2)]

    def start(copies):
        for c in copies:
            c.start()

    def wait(copies):
        for c in copies:
            c.wait()

    e_copies = [pltpu.make_async_copy(e_hbm.at[pl.ds(lo, size)], e_in.at[pl.ds(lo, size)], e_sem.at[k]) for k, (lo, size) in enumerate(parts)]
    start(e_copies)
    for t in range(len(parts)):
        start(z_copies(0, t))

    barrier = pltpu.get_barrier_semaphore()
    for r in range(1, n):
        pl.semaphore_signal(barrier, inc=1, device_id={"tp": lax.rem(me + r, n)}, device_id_type=MESH)
    for c, (lo, size) in zip(e_copies, parts):
        c.wait()
        e_t[:, lo:lo + size] = e_in[lo:lo + size, :].T
    pl.semaphore_wait(barrier, n - 1)

    def pair_copy(u):
        return pltpu.make_async_remote_copy(src_ref=to_pair.at[lax.rem(u, 2)], dst_ref=from_pair.at[u], send_sem=pair_send.at[u],
                                            recv_sem=pair_recv.at[u], device_id={"tp": partner}, device_id_type=MESH)

    def ring_copy(u):
        return pltpu.make_async_remote_copy(src_ref=to_ring.at[lax.rem(u, 2)], dst_ref=from_ring.at[u], send_sem=ring_send.at[u],
                                            recv_sem=ring_recv.at[u], device_id={"tp": ahead}, device_id_type=MESH)

    def combine(u):
        slot = lax.rem(u, 2)
        pair_copy(u).wait_recv()

        @pl.when(u < 2)
        def _():
            to_ring[slot] = own_part[slot] + from_pair[u]
            ring_copy(u).start()

        @pl.when((u >= 2) & (u < rounds - 2))
        def _():
            ring_copy(u - 2).wait()
            to_ring[slot] = own_part[slot] + from_pair[u] + from_ring[u - 2]
            ring_copy(u).start()

        @pl.when(u >= rounds - 2)
        def _():
            ring_copy(u - 2).wait()
            to_ring[slot] = own_part[slot] + from_pair[u] + from_ring[u - 2]

    def body(u, carry):
        slot = lax.rem(u, 2)
        both = [block_of(u, own) * 2 + slot for own in range(2)]
        stats = [(lse[row], scale[row], tgt[row]) for row in both]
        for t, (first, count) in enumerate(parts):
            z, dz = z_bufs[t], dz_bufs[t]

            @pl.when(u > 0)
            def _():
                wait(dz_copies(u - 1, t))

            wait(z_copies(u, t))
            for lo, size in row_chunks(count, DZ_ROWS):
                rows = lax.broadcasted_iota(jnp.int32, (size, half), 0) + lo
                for own, (l, sc, want) in enumerate(stats):
                    hot = jnp.where(rows == want - first, 1.0, 0.0)
                    dz[own, lo:lo + size, :] = ((jnp.exp(z[own, lo:lo + size, :] - l) - hot) * sc).astype(jnp.bfloat16)
            both_dz = jnp.concatenate([dz[0], dz[1]], axis=1)
            part = jnp.dot(e_t[:, first:first + count], both_dz, preferred_element_type=jnp.float32)
            acc[...] = part if t == 0 else acc[...] + part
            start(dz_copies(u, t))

            @pl.when(u < rounds - 1)
            def _():
                start(z_copies(u + 1, t))

        @pl.when(u > 0)
        def _():
            combine(u - 1)

        @pl.when(u >= 2)
        def _():
            pair_copy(u - 2).wait_send()
        to_pair[slot] = acc[:, :half]
        own_part[slot] = acc[:, half:]
        pair_copy(u).start()
        return carry

    lax.fori_loop(0, rounds, body, 0)
    combine(rounds - 1)
    for u in (rounds - 2, rounds - 1):
        pair_copy(u).wait_send()
    for t in range(len(parts)):
        wait(dz_copies(rounds - 1, t))

    d_x = jnp.concatenate([to_ring[0].T, to_ring[1].T], axis=0)
    rows = hid[...].astype(jnp.float32)
    centered = rows - jnp.mean(rows, axis=-1, keepdims=True)
    rstd = lax.rsqrt(jnp.mean(centered * centered, axis=-1, keepdims=True) + LN_EPS)
    normed = centered * rstd
    d_ln[me] = jnp.concatenate([jnp.sum(d_x * normed, axis=0, keepdims=True), jnp.sum(d_x, axis=0, keepdims=True)], axis=0)

    def ln_copy(r, slot, peer):
        return pltpu.make_async_remote_copy(src_ref=d_ln.at[slot], dst_ref=d_ln.at[slot], send_sem=ln_send.at[r - 1],
                                            recv_sem=ln_recv.at[r - 1], device_id={"tp": peer}, device_id_type=MESH)

    d_normed = d_x * lnp[0:1, :]
    proj = jnp.mean(d_normed * normed, axis=-1, keepdims=True)
    dh_o[...] = (rstd * (d_normed - jnp.mean(d_normed, axis=-1, keepdims=True) - normed * proj)).astype(jnp.bfloat16)
    for r in range(1, n):
        ln_copy(r, me, lax.rem(me + r, n)).start()
    for r in range(1, n):
        src = lax.rem(me + n - r, n)
        ln_copy(r, src, src).wait()
    grad = d_ln[0]
    for d in range(1, n):
        grad = grad + d_ln[d]
    dln_o[...] = grad


def backward(n, hidden, ln_params, lse, scale, tgt, z, out_embed):
    tok, dim = hidden.shape
    vocab = out_embed.shape[0]
    half = tok // 2
    f32, bf16 = jnp.float32, jnp.bfloat16
    vmem = pl.BlockSpec(memory_space=pltpu.VMEM)
    hbm = pl.BlockSpec(memory_space=pl.ANY)
    dma = pltpu.SemaphoreType.DMA
    return pl.pallas_call(
        functools.partial(backward_kernel, n),
        name="backward",
        out_shape=(
            jax.ShapeDtypeStruct((2 * n, vocab, half), bf16),
            jax.ShapeDtypeStruct((tok, dim), bf16),
            jax.ShapeDtypeStruct((2, dim), f32),
        ),
        in_specs=[vmem] * 5 + [hbm, hbm],
        out_specs=(hbm, vmem, vmem),
        scratch_shapes=[pltpu.VMEM((2, size, half), f32) for _, size in vocab_parts(vocab)] + [pltpu.VMEM((2, size, half), bf16) for _, size in vocab_parts(vocab)] + [
            pltpu.VMEM((vocab, dim), bf16),
            pltpu.VMEM((dim, vocab), bf16),
            pltpu.VMEM((dim, tok), f32),
            pltpu.VMEM((2, dim, half), f32),
            pltpu.VMEM((2, dim, half), f32),
            pltpu.VMEM((n, dim, half), f32),
            pltpu.VMEM((2, dim, half), f32),
            pltpu.VMEM((n - 2, dim, half), f32),
            pltpu.VMEM((n, 2, dim), f32),
            dma((3, 2)), dma((3, 2)), dma((3,)),
            dma((n,)), dma((n,)), dma((n - 2,)), dma((n - 2,)), dma((n - 1,)), dma((n - 1,)),
        ],
        compiler_params=pltpu.CompilerParams(collective_id=1, has_side_effects=True, vmem_limit_bytes=66_000_000),
        cost_estimate=pl.CostEstimate(flops=2 * n * tok * dim * vocab, bytes_accessed=6 * n * tok * vocab, transcendentals=n * tok * vocab),
    )(hidden, ln_params, lse, scale, tgt, z, out_embed)


def update_kernel(dz, x, e, m, v, e_o, m_o, v_o, grad):
    all_dz = jnp.concatenate([dz[j] for j in range(dz.shape[0])], axis=1)
    grad[...] = jnp.dot(all_dz, x[...], preferred_element_type=jnp.float32)
    for lo, size in row_chunks(grad.shape[0], ADAM_ROWS):
        part = slice(lo, lo + size)
        new_e, m_o[part, :], v_o[part, :] = adam_step(e[part, :].astype(jnp.float32), grad[part, :], m[part, :], v[part, :], WEIGHT_DECAY)
        e_o[part, :] = new_e.astype(jnp.bfloat16)


def update(dz, x, out_embed, mom1, mom2):
    vocab, dim = out_embed.shape
    toks = x.shape[0]
    vt = 640
    f32, bf16 = jnp.float32, jnp.bfloat16
    tile = pl.BlockSpec((vt, dim), lambda i: (i, 0))
    return pl.pallas_call(
        update_kernel,
        name="update",
        grid=(pl.cdiv(vocab, vt),),
        in_specs=[pl.BlockSpec((dz.shape[0], vt, dz.shape[2]), lambda i: (0, i, 0)), pl.BlockSpec((toks, dim), lambda i: (0, 0)), tile, tile, tile],
        out_specs=(tile, tile, tile),
        out_shape=(jax.ShapeDtypeStruct((vocab, dim), bf16), jax.ShapeDtypeStruct((vocab, dim), f32), jax.ShapeDtypeStruct((vocab, dim), f32)),
        scratch_shapes=[pltpu.VMEM((vt, dim), f32)],
        compiler_params=pltpu.CompilerParams(vmem_limit_bytes=VMEM_LIMIT, dimension_semantics=("arbitrary",)),
        cost_estimate=pl.CostEstimate(flops=2 * toks * dim * vocab, bytes_accessed=2 * toks * vocab + 20 * vocab * dim, transcendentals=2 * vocab * dim),
    )(dz, x, out_embed, mom1, mom2)


def solution(mesh):
    n = mesh.shape["tp"]
    row_spec = P(("dp", "tp"), None)
    tok_spec = P(("dp", "tp"))
    vocab_spec = P("tp", None)
    repl_spec = P()
    part_spec = P("dp", None)

    def device_step(hidden, targets, loss_mask, ln_params, out_embed, ln_mom1, ln_mom2, embed_mom1, embed_mom2):
        tok, dim = hidden.shape
        tm = jnp.stack([targets, loss_mask])
        z, x_full, lse, scale, tgt, loss, mean = forward(n, hidden, tm, ln_params, out_embed)
        dz, d_hidden, d_ln = backward(n, hidden, ln_params, lse, scale, tgt, z, out_embed)
        ln_new, ln_mom1_new, ln_mom2_new = adam_step(ln_params, d_ln, ln_mom1, ln_mom2, 0.0)
        embed_new, embed_mom1_new, embed_mom2_new = update(dz, x_full.reshape(n * tok, dim), out_embed, embed_mom1, embed_mom2)
        return (loss.reshape(tok), mean[0, :1], d_hidden, ln_new, ln_mom1_new, ln_mom2_new, embed_new, embed_mom1_new, embed_mom2_new)

    return jax.shard_map(device_step, mesh=mesh, in_specs=(row_spec, tok_spec, tok_spec, repl_spec, vocab_spec, repl_spec, repl_spec, vocab_spec, vocab_spec), out_specs=(tok_spec, P("dp"), row_spec, part_spec, part_spec, part_spec, row_spec, row_spec, row_spec), check_vma=False)
```

```python
import functools

import jax
import jax.numpy as jnp
from jax import lax
from jax.experimental import pallas as pl
from jax.experimental.pallas import tpu as pltpu
from jax.sharding import PartitionSpec as P

LN_EPS = 1e-5
BETA_ONE = 0.9
BETA_TWO = 0.95
ADAM_EPS = 1e-8
LEARN_RATE = 1e-3
WEIGHT_DECAY = 0.1
ADAM_STEP = 10

MESH = pl.DeviceIdType.MESH
VMEM_LIMIT = 64_000_000
NEG = -3.0e38
STAT_ROWS = 32
ADAM_ROWS = 16
DZ_ROWS = 64
DOT_ROWS = 1056


def layer_norm(hidden, ln_params):
    rows_f32 = hidden.astype(jnp.float32)
    row_mean = jnp.mean(rows_f32, axis=-1, keepdims=True)
    centered = rows_f32 - row_mean
    row_var = jnp.mean(centered * centered, axis=-1, keepdims=True)
    normed = centered * lax.rsqrt(row_var + LN_EPS)
    return normed * ln_params[0:1] + ln_params[1:2]


def adam_step(param_val, grad_val, m_old, v_old, decay_rate):
    m_new = BETA_ONE * m_old + (1.0 - BETA_ONE) * grad_val
    v_new = BETA_TWO * v_old + (1.0 - BETA_TWO) * grad_val * grad_val
    m_step = m_new * (LEARN_RATE / (1.0 - BETA_ONE ** ADAM_STEP))
    v_hat = v_new * (1.0 / (1.0 - BETA_TWO ** ADAM_STEP))
    new_param = (1.0 - LEARN_RATE * decay_rate) * param_val - m_step / (jnp.sqrt(v_hat) + ADAM_EPS)
    return new_param, m_new, v_new


def row_chunks(rows, size):
    return [(lo, min(size, rows - lo)) for lo in range(0, rows, size)]


def forward_kernel(n, tiles, hid, tm, lnp, e_hbm,
                   z_hbm, x_hbm, lse_o, scale_o, tgt_o, loss_o, mean_o,
                   x_all, x_send, tm_all, e_v, x_t, z_a, z_b, m_run, m_old, s_run, t_run, st_own, st_all,
                   e_sem, z_sem, xo_sem, sx_send, sx_recv, tm_send, tm_recv, st_send, st_recv):
    me = lax.axis_index("tp")
    chips = n // 2
    chip, core = me // 2, lax.rem(me, 2)
    sgn = 1 - 2 * core
    tok = hid.shape[0]
    vocab = e_hbm.shape[0]
    vt = vocab // tiles

    def dev(chip_idx, core_idx):
        return lax.rem(chip_idx + 2 * chips, chips) * 2 + core_idx

    e_copies = [pltpu.make_async_copy(e_hbm.at[pl.ds(t * vt, vt)], e_v.at[pl.ds(t * vt, vt)], e_sem.at[t]) for t in range(tiles)]
    for c in e_copies:
        c.start()

    barrier = pltpu.get_barrier_semaphore()
    for r in range(1, n):
        pl.semaphore_signal(barrier, inc=1, device_id={"tp": lax.rem(me + r, n)}, device_id_type=MESH)

    x_send[...] = layer_norm(hid[...], lnp[...]).astype(jnp.bfloat16)
    x_all[me] = x_send[...]
    tm_all[me] = tm[...]
    pl.semaphore_wait(barrier, n - 1)

    def xcopy(idx, src, slot, dst, recv):
        return pltpu.make_async_remote_copy(src_ref=src, dst_ref=x_all.at[slot], send_sem=sx_send.at[idx],
                                            recv_sem=sx_recv.at[recv], device_id={"tp": dst}, device_id_type=MESH)

    partner = dev(chip, 1 - core)
    ahead = dev(chip + sgn, core)
    behind = dev(chip - sgn, core)
    a1 = dev(chip - sgn, core)
    a2 = dev(chip + sgn, core)
    far = dev(chip + 2, core)
    s0 = xcopy(0, x_send, me, partner, 1)
    s1 = xcopy(1, x_send, me, ahead, 2)
    s2 = xcopy(2, x_send, me, behind, 4)
    s3 = xcopy(3, x_all.at[a1], a1, partner, 3)
    s4 = xcopy(4, x_all.at[a1], a1, ahead, 6)
    s5 = xcopy(5, x_all.at[a2], a2, partner, 5)
    s6 = xcopy(6, x_all.at[far], far, partner, 7)

    def tmcopy(r):
        peer = lax.rem(me + r, n)
        return pltpu.make_async_remote_copy(src_ref=tm, dst_ref=tm_all.at[me], send_sem=tm_send.at[r - 1],
                                            recv_sem=tm_recv.at[r - 1], device_id={"tp": peer}, device_id_type=MESH)

    tm_copies = [tmcopy(r) for r in range(1, n)]
    s0.start()
    for c in tm_copies:
        c.start()
    s1.start()

    def block_of(p):
        q = lax.rem(p, 2)
        h = p // 2
        own_core = core + q * sgn
        step = jnp.where(h == 0, 0, jnp.where(h == 1, -sgn, jnp.where(h == 2, sgn, 2)))
        flip = jnp.where(h == 3, 1, 1 - 2 * q)
        return dev(chip + step * flip, own_core)

    def z_copy(nn, buf):
        p, t = nn // tiles, lax.rem(nn, tiles)
        slot = lax.rem(nn, 2)
        return pltpu.make_async_copy(buf, z_hbm.at[pl.ds(2 * block_of(p), 2), pl.ds(pl.multiple_of(t * vt, 16), vt)], z_sem.at[slot])

    def x_out(p):
        b = block_of(p)
        return pltpu.make_async_copy(x_all.at[b], x_hbm.at[b], xo_sem.at[p])

    def reset():
        m_run[...] = jnp.full_like(m_run, NEG)
        m_old[...] = jnp.full_like(m_old, NEG)
        s_run[...] = jnp.zeros_like(s_run)
        t_run[...] = jnp.zeros_like(t_run)

    sub = lax.broadcasted_iota(jnp.int32, (8, tok), 0)

    def sums_begin(nn):
        p, t = nn // tiles, lax.rem(nn, tiles)
        want = tm_all[block_of(p)][0:1] - (me * vocab + t * vt) - sub
        m = m_run[...]
        return want, m, s_run[...] * jnp.exp(m_old[...] - m), t_run[...]

    def sums_rows(acc, buf, start, count):
        want, m, s, tgt = acc
        for lo, size in row_chunks(count, STAT_ROWS):
            part = slice(start + lo, start + lo + size)
            z = jnp.concatenate([buf[0, part, :], buf[1, part, :]], axis=1).reshape(size // 8, 8, tok)
            s = s + jnp.sum(jnp.exp(z - m[None]), axis=0)
            rows = lax.broadcasted_iota(jnp.int32, z.shape, 0) * 8 + (start + lo)
            tgt = tgt + jnp.sum(jnp.where(want[None] == rows, z, 0.0), axis=0)
        return want, m, s, tgt

    def sums_end(acc):
        _, m_old[...], s_run[...], t_run[...] = acc

    def sums(nn, buf):
        sums_end(sums_rows(sums_begin(nn), buf, 0, vt))

    def st_copy(r, blk):
        peer = lax.rem(me + r, n)
        return pltpu.make_async_remote_copy(src_ref=st_own.at[blk], dst_ref=st_all.at[me, blk], send_sem=st_send.at[r - 1],
                                            recv_sem=st_recv.at[r - 1], device_id={"tp": peer}, device_id_type=MESH)

    def finish(p):
        b = block_of(p)
        m, s = m_run[...], s_run[...]
        m_all = jnp.max(m, axis=0, keepdims=True)
        s_sum = jnp.sum(s * jnp.exp(m - m_all), axis=0, keepdims=True)
        both = jnp.concatenate([m_all + jnp.log(s_sum), jnp.sum(t_run[...], axis=0, keepdims=True)], axis=0)
        st_own[b] = both
        st_all[me, b] = both

    def send_stats(p):
        b = block_of(p)
        for r in range(1, n):
            st_copy(r, b).start()

    reset()

    def step(nn, cur, prev):
        p, t = nn // tiles, lax.rem(nn, tiles)

        @pl.when(t == 0)
        def _():
            @pl.when(p == 1)
            def _():
                for c in tm_copies:
                    c.wait()
                s0.wait_recv()

            @pl.when(p == 2)
            def _():
                s1.wait()
                s3.start()
                s2.start()

            @pl.when(p == 3)
            def _():
                s3.wait_recv()
                s4.start()

            @pl.when(p == 4)
            def _():
                s2.wait()
                s5.start()

            @pl.when(p == 5)
            def _():
                s5.wait_recv()

            @pl.when(p == 6)
            def _():
                s4.wait_recv()
                s6.start()

            @pl.when(p == 7)
            def _():
                s6.wait_recv()

            b = block_of(p)
            x_out(p).start()
            x_t[...] = x_all[b].T

        for tt in range(tiles):
            @pl.when(nn == tt)
            def _():
                e_copies[tt].wait()

        @pl.when(nn >= 2)
        def _():
            z_copy(nn - 2, cur).wait()

        top = jnp.full((8, tok), NEG, jnp.float32)
        acc = sums_begin(jnp.maximum(nn - 1, 0))
        for lo, size in row_chunks(vt, DOT_ROWS):
            z = jnp.dot(e_v[pl.ds(pl.multiple_of(t * vt + lo, 16), size), :], x_t[...], preferred_element_type=jnp.float32)
            cur[0, lo:lo + size, :] = z[:, :tok // 2]
            cur[1, lo:lo + size, :] = z[:, tok // 2:]
            top = jnp.maximum(top, jnp.max(z.reshape(size // 8, 8, tok), axis=0))
            acc = sums_rows(acc, prev, lo, size)
        sums_end(acc)
        z_copy(nn, cur).start()

        @pl.when(t == 0)
        def _():
            @pl.when(nn > 0)
            def _():
                finish(p - 1)
            reset()

        m_run[...] = jnp.maximum(m_run[...], top)

        @pl.when((t == 1) & (p > 0))
        def _():
            send_stats(p - 1)

    def body(i, carry):
        step(2 * i, z_a, z_b)
        step(2 * i + 1, z_b, z_a)
        return carry

    total = n * tiles
    lax.fori_loop(0, total // 2, body, 0)
    sums(total - 1, z_b)
    finish(n - 1)
    z_copy(total - 2, z_a).wait()
    send_stats(n - 1)
    z_copy(total - 1, z_b).wait()
    s0.wait_send()
    s3.wait_send()
    s4.wait_send()
    s5.wait_send()
    s6.wait_send()
    for p in range(n):
        x_out(p).wait()

    for r in range(1, n):
        src = lax.rem(me + n - r, n)
        pltpu.make_async_remote_copy(src_ref=st_own, dst_ref=st_all.at[src], send_sem=st_send.at[r - 1],
                                     recv_sem=st_recv.at[r - 1], device_id={"tp": src}, device_id_type=MESH).wait()

    parts = [st_all[d] for d in range(n)]
    lses = [q[:, 0, :] for q in parts]
    top = functools.reduce(jnp.maximum, lses)
    lse = top + jnp.log(sum(jnp.exp(q - top) for q in lses))
    tgt_logit = sum(q[:, 1, :] for q in parts)
    tm_full = tm_all[...]
    mask = tm_full[:, 1, :].astype(jnp.float32)
    count = jnp.sum(mask)
    loss = (lse - tgt_logit) * mask
    half = tok // 2
    for d in range(n):
        for h in range(2):
            part = slice(h * half, (h + 1) * half)
            lse_o[2 * d + h] = lse[d:d + 1, part]
            scale_o[2 * d + h] = mask[d:d + 1, part] / count
            tgt_o[2 * d + h] = tm_full[d, 0:1, part] - me * vocab
    own = lax.broadcasted_iota(jnp.int32, loss.shape, 0) == me
    loss_o[...] = jnp.sum(jnp.where(own, loss, 0.0), axis=0, keepdims=True)
    mean_o[...] = jnp.full(mean_o.shape, jnp.sum(loss) / count, jnp.float32)


def forward(n, hidden, tm, ln_params, out_embed):
    tok, dim = hidden.shape
    vocab = out_embed.shape[0]
    tiles = 3
    vt = vocab // tiles
    vmem = pl.BlockSpec(memory_space=pltpu.VMEM)
    hbm = pl.BlockSpec(memory_space=pl.ANY)
    f32, bf16, i32 = jnp.float32, jnp.bfloat16, jnp.int32
    dma = pltpu.SemaphoreType.DMA
    return pl.pallas_call(
        functools.partial(forward_kernel, n, tiles),
        name="forward",
        out_shape=(
            jax.ShapeDtypeStruct((2 * n, vocab, tok // 2), f32),
            jax.ShapeDtypeStruct((n, tok, dim), bf16),
            jax.ShapeDtypeStruct((2 * n, 1, tok // 2), f32),
            jax.ShapeDtypeStruct((2 * n, 1, tok // 2), f32),
            jax.ShapeDtypeStruct((2 * n, 1, tok // 2), i32),
            jax.ShapeDtypeStruct((1, tok), f32),
            jax.ShapeDtypeStruct((1, 128), f32),
        ),
        in_specs=[vmem, vmem, vmem, hbm],
        out_specs=(hbm, hbm, vmem, vmem, vmem, vmem, vmem),
        scratch_shapes=[
            pltpu.VMEM((n, tok, dim), bf16),
            pltpu.VMEM((tok, dim), bf16),
            pltpu.VMEM((n, 2, tok), i32),
            pltpu.VMEM((vocab, dim), bf16),
            pltpu.VMEM((dim, tok), bf16),
            pltpu.VMEM((2, vt, tok // 2), f32),
            pltpu.VMEM((2, vt, tok // 2), f32),
            pltpu.VMEM((8, tok), f32),
            pltpu.VMEM((8, tok), f32),
            pltpu.VMEM((8, tok), f32),
            pltpu.VMEM((8, tok), f32),
            pltpu.VMEM((n, 2, tok), f32),
            pltpu.VMEM((n, n, 2, tok), f32),
            dma((tiles,)), dma((2,)), dma((n,)),
            dma((7,)), dma((8,)), dma((n - 1,)), dma((n - 1,)), dma((n - 1,)), dma((n - 1,)),
        ],
        compiler_params=pltpu.CompilerParams(collective_id=0, has_side_effects=True, vmem_limit_bytes=VMEM_LIMIT),
        cost_estimate=pl.CostEstimate(flops=2 * n * tok * dim * vocab, bytes_accessed=4 * n * tok * vocab, transcendentals=n * tok * vocab),
    )(hidden, tm, ln_params, out_embed)


def vocab_parts(vocab):
    size = vocab // 3 // 256 * 256
    return [(0, size), (size, size), (2 * size, vocab - 2 * size)]


def backward_kernel(n, hid, lnp, lse, scale, tgt, z_hbm, e_hbm,
                    dz_hbm, dh_o, dln_o,
                    z_0, z_1, z_2, dz_0, dz_1, dz_2, e_in, e_t, acc, own_part, to_pair, from_pair, to_ring, from_ring, d_ln,
                    z_sem, dz_sem, e_sem, pair_send, pair_recv, ring_send, ring_recv, ln_send, ln_recv):
    me = lax.axis_index("tp")
    chips = n // 2
    chip, core = me // 2, lax.rem(me, 2)
    sgn = 1 - 2 * core
    vocab, half = e_in.shape[0], acc.shape[1] // 2
    z_bufs, dz_bufs = (z_0, z_1, z_2), (dz_0, dz_1, dz_2)
    parts = vocab_parts(vocab)
    rounds = 2 * chips

    def dev(chip_idx, core_idx):
        return lax.rem(chip_idx + 2 * chips, chips) * 2 + core_idx

    partner = dev(chip, 1 - core)
    ahead = dev(chip + sgn, core)

    def block_of(u, own):
        hop = 1 + u // 2
        return dev(chip - sgn * hop, core) if own else dev(chip + sgn * hop, 1 - core)

    def z_copies(u, t):
        lo, size = parts[t]
        return [pltpu.make_async_copy(z_hbm.at[block_of(u, own) * 2 + lax.rem(u, 2), pl.ds(lo, size)], z_bufs[t].at[own], z_sem.at[t, own])
                for own in range(2)]

    def dz_copies(u, t):
        lo, size = parts[t]
        return [pltpu.make_async_copy(dz_bufs[t].at[own], dz_hbm.at[block_of(u, own) * 2 + lax.rem(u, 2), pl.ds(lo, size)], dz_sem.at[t, own])
                for own in range(2)]

    def start(copies):
        for c in copies:
            c.start()

    def wait(copies):
        for c in copies:
            c.wait()

    e_copies = [pltpu.make_async_copy(e_hbm.at[pl.ds(lo, size)], e_in.at[pl.ds(lo, size)], e_sem.at[k]) for k, (lo, size) in enumerate(parts)]
    start(e_copies)
    for t in range(len(parts)):
        start(z_copies(0, t))

    barrier = pltpu.get_barrier_semaphore()
    for r in range(1, n):
        pl.semaphore_signal(barrier, inc=1, device_id={"tp": lax.rem(me + r, n)}, device_id_type=MESH)
    for c, (lo, size) in zip(e_copies, parts):
        c.wait()
        e_t[:, lo:lo + size] = e_in[lo:lo + size, :].T
    pl.semaphore_wait(barrier, n - 1)

    def pair_copy(u):
        return pltpu.make_async_remote_copy(src_ref=to_pair.at[lax.rem(u, 2)], dst_ref=from_pair.at[u], send_sem=pair_send.at[u],
                                            recv_sem=pair_recv.at[u], device_id={"tp": partner}, device_id_type=MESH)

    def ring_copy(u):
        return pltpu.make_async_remote_copy(src_ref=to_ring.at[lax.rem(u, 2)], dst_ref=from_ring.at[u], send_sem=ring_send.at[u],
                                            recv_sem=ring_recv.at[u], device_id={"tp": ahead}, device_id_type=MESH)

    def combine(u):
        slot = lax.rem(u, 2)
        pair_copy(u).wait_recv()

        @pl.when(u < 2)
        def _():
            to_ring[slot] = own_part[slot] + from_pair[u]
            ring_copy(u).start()

        @pl.when((u >= 2) & (u < rounds - 2))
        def _():
            ring_copy(u - 2).wait()
            to_ring[slot] = own_part[slot] + from_pair[u] + from_ring[u - 2]
            ring_copy(u).start()

        @pl.when(u >= rounds - 2)
        def _():
            ring_copy(u - 2).wait()
            to_ring[slot] = own_part[slot] + from_pair[u] + from_ring[u - 2]

    def body(u, carry):
        slot = lax.rem(u, 2)
        both = [block_of(u, own) * 2 + slot for own in range(2)]
        stats = [(lse[row], scale[row], tgt[row]) for row in both]
        for t, (first, count) in enumerate(parts):
            z, dz = z_bufs[t], dz_bufs[t]

            @pl.when(u > 0)
            def _():
                wait(dz_copies(u - 1, t))

            wait(z_copies(u, t))
            for lo, size in row_chunks(count, DZ_ROWS):
                rows = lax.broadcasted_iota(jnp.int32, (size, half), 0) + lo
                for own, (l, sc, want) in enumerate(stats):
                    hot = jnp.where(rows == want - first, 1.0, 0.0)
                    dz[own, lo:lo + size, :] = ((jnp.exp(z[own, lo:lo + size, :] - l) - hot) * sc).astype(jnp.bfloat16)
            both_dz = jnp.concatenate([dz[0], dz[1]], axis=1)
            part = jnp.dot(e_t[:, first:first + count], both_dz, preferred_element_type=jnp.float32)
            acc[...] = part if t == 0 else acc[...] + part
            start(dz_copies(u, t))

            @pl.when(u < rounds - 1)
            def _():
                start(z_copies(u + 1, t))

        @pl.when(u > 0)
        def _():
            combine(u - 1)

        @pl.when(u >= 2)
        def _():
            pair_copy(u - 2).wait_send()
        to_pair[slot] = acc[:, :half]
        own_part[slot] = acc[:, half:]
        pair_copy(u).start()
        return carry

    lax.fori_loop(0, rounds, body, 0)
    combine(rounds - 1)
    for u in (rounds - 2, rounds - 1):
        pair_copy(u).wait_send()
    for t in range(len(parts)):
        wait(dz_copies(rounds - 1, t))

    d_x = jnp.concatenate([to_ring[0].T, to_ring[1].T], axis=0)
    rows = hid[...].astype(jnp.float32)
    centered = rows - jnp.mean(rows, axis=-1, keepdims=True)
    rstd = lax.rsqrt(jnp.mean(centered * centered, axis=-1, keepdims=True) + LN_EPS)
    normed = centered * rstd
    d_ln[me] = jnp.concatenate([jnp.sum(d_x * normed, axis=0, keepdims=True), jnp.sum(d_x, axis=0, keepdims=True)], axis=0)

    def ln_copy(r, slot, peer):
        return pltpu.make_async_remote_copy(src_ref=d_ln.at[slot], dst_ref=d_ln.at[slot], send_sem=ln_send.at[r - 1],
                                            recv_sem=ln_recv.at[r - 1], device_id={"tp": peer}, device_id_type=MESH)

    d_normed = d_x * lnp[0:1, :]
    proj = jnp.mean(d_normed * normed, axis=-1, keepdims=True)
    dh_o[...] = (rstd * (d_normed - jnp.mean(d_normed, axis=-1, keepdims=True) - normed * proj)).astype(jnp.bfloat16)
    for r in range(1, n):
        ln_copy(r, me, lax.rem(me + r, n)).start()
    for r in range(1, n):
        src = lax.rem(me + n - r, n)
        ln_copy(r, src, src).wait()
    grad = d_ln[0]
    for d in range(1, n):
        grad = grad + d_ln[d]
    dln_o[...] = grad


def backward(n, hidden, ln_params, lse, scale, tgt, z, out_embed):
    tok, dim = hidden.shape
    vocab = out_embed.shape[0]
    half = tok // 2
    f32, bf16 = jnp.float32, jnp.bfloat16
    vmem = pl.BlockSpec(memory_space=pltpu.VMEM)
    hbm = pl.BlockSpec(memory_space=pl.ANY)
    dma = pltpu.SemaphoreType.DMA
    return pl.pallas_call(
        functools.partial(backward_kernel, n),
        name="backward",
        out_shape=(
            jax.ShapeDtypeStruct((2 * n, vocab, half), bf16),
            jax.ShapeDtypeStruct((tok, dim), bf16),
            jax.ShapeDtypeStruct((2, dim), f32),
        ),
        in_specs=[vmem] * 5 + [hbm, hbm],
        out_specs=(hbm, vmem, vmem),
        scratch_shapes=[pltpu.VMEM((2, size, half), f32) for _, size in vocab_parts(vocab)] + [pltpu.VMEM((2, size, half), bf16) for _, size in vocab_parts(vocab)] + [
            pltpu.VMEM((vocab, dim), bf16),
            pltpu.VMEM((dim, vocab), bf16),
            pltpu.VMEM((dim, tok), f32),
            pltpu.VMEM((2, dim, half), f32),
            pltpu.VMEM((2, dim, half), f32),
            pltpu.VMEM((n, dim, half), f32),
            pltpu.VMEM((2, dim, half), f32),
            pltpu.VMEM((n - 2, dim, half), f32),
            pltpu.VMEM((n, 2, dim), f32),
            dma((3, 2)), dma((3, 2)), dma((3,)),
            dma((n,)), dma((n,)), dma((n - 2,)), dma((n - 2,)), dma((n - 1,)), dma((n - 1,)),
        ],
        compiler_params=pltpu.CompilerParams(collective_id=1, has_side_effects=True, vmem_limit_bytes=66_000_000),
        cost_estimate=pl.CostEstimate(flops=2 * n * tok * dim * vocab, bytes_accessed=6 * n * tok * vocab, transcendentals=n * tok * vocab),
    )(hidden, ln_params, lse, scale, tgt, z, out_embed)


def update_kernel(dz, x, e, m, v, e_o, m_o, v_o, grad):
    all_dz = jnp.concatenate([dz[j] for j in range(dz.shape[0])], axis=1)
    grad[...] = jnp.dot(all_dz, x[...], preferred_element_type=jnp.float32)
    for lo, size in row_chunks(grad.shape[0], ADAM_ROWS):
        part = slice(lo, lo + size)
        new_e, m_o[part, :], v_o[part, :] = adam_step(e[part, :].astype(jnp.float32), grad[part, :], m[part, :], v[part, :], WEIGHT_DECAY)
        e_o[part, :] = new_e.astype(jnp.bfloat16)


def update(dz, x, out_embed, mom1, mom2):
    vocab, dim = out_embed.shape
    toks = x.shape[0]
    vt = 800
    f32, bf16 = jnp.float32, jnp.bfloat16
    tile = pl.BlockSpec((vt, dim), lambda i: (i, 0))
    return pl.pallas_call(
        update_kernel,
        name="update",
        grid=(pl.cdiv(vocab, vt),),
        in_specs=[pl.BlockSpec((dz.shape[0], vt, dz.shape[2]), lambda i: (0, i, 0)), pl.BlockSpec((toks, dim), lambda i: (0, 0)), tile, tile, tile],
        out_specs=(tile, tile, tile),
        out_shape=(jax.ShapeDtypeStruct((vocab, dim), bf16), jax.ShapeDtypeStruct((vocab, dim), f32), jax.ShapeDtypeStruct((vocab, dim), f32)),
        scratch_shapes=[pltpu.VMEM((vt, dim), f32)],
        compiler_params=pltpu.CompilerParams(vmem_limit_bytes=VMEM_LIMIT, dimension_semantics=("arbitrary",)),
        cost_estimate=pl.CostEstimate(flops=2 * toks * dim * vocab, bytes_accessed=2 * toks * vocab + 20 * vocab * dim, transcendentals=2 * vocab * dim),
    )(dz, x, out_embed, mom1, mom2)


def solution(mesh):
    n = mesh.shape["tp"]
    row_spec = P(("dp", "tp"), None)
    tok_spec = P(("dp", "tp"))
    vocab_spec = P("tp", None)
    repl_spec = P()
    part_spec = P("dp", None)

    def device_step(hidden, targets, loss_mask, ln_params, out_embed, ln_mom1, ln_mom2, embed_mom1, embed_mom2):
        tok, dim = hidden.shape
        tm = jnp.stack([targets, loss_mask])
        z, x_full, lse, scale, tgt, loss, mean = forward(n, hidden, tm, ln_params, out_embed)
        dz, d_hidden, d_ln = backward(n, hidden, ln_params, lse, scale, tgt, z, out_embed)
        ln_new, ln_mom1_new, ln_mom2_new = adam_step(ln_params, d_ln, ln_mom1, ln_mom2, 0.0)
        embed_new, embed_mom1_new, embed_mom2_new = update(dz, x_full.reshape(n * tok, dim), out_embed, embed_mom1, embed_mom2)
        return (loss.reshape(tok), mean[0, :1], d_hidden, ln_new, ln_mom1_new, ln_mom2_new, embed_new, embed_mom1_new, embed_mom2_new)

    return jax.shard_map(device_step, mesh=mesh, in_specs=(row_spec, tok_spec, tok_spec, repl_spec, vocab_spec, repl_spec, repl_spec, vocab_spec, vocab_spec), out_specs=(tok_spec, P("dp"), row_spec, part_spec, part_spec, part_spec, row_spec, row_spec, row_spec), check_vma=False)
```
